32 devices in a mesh: replica: 4 (over y, core), shard: 8 (over z, x).
Axes of the slice: x: 2, y: 2, z: 4, core: 2. Of those that a mesh axis runs over, the one named last changes fastest.
Arguments:
- anchor: float32 [384, 8192], P('shard'), may hold values from -6 to 6
- replica_rows: bfloat16 [4, 384, 8192], P('replica', 'shard'), may hold values from -6 to 6
- outer_velocity: float32 [384, 8192], P('shard', 'replica'), may hold values from -6 to 6
- features: bfloat16 [4, 384, 256], P('replica', 'shard'), may hold values from -6 to 6
- cotangent: bfloat16 [4, 256, 1024], P('replica', 'shard'), may hold values from -0.375 to 0.375
- inner_weight: float32 [4, 384, 1024], P('replica', 'shard'), may hold values from -6 to 6
- first_moment: float32 [4, 384, 1024], P('replica', 'shard'), may hold values from -6 to 6
- second_moment: float32 [4, 384, 1024], P('replica', 'shard'), may hold values from 0.5 to 2
Outputs:
- new_anchor: float32 [384, 8192], P('shard')
- merged_rows: bfloat16 [4, 384, 8192], P('replica', 'shard')
- new_velocity: float32 [384, 8192], P('shard', 'replica')
- new_weight: float32 [4, 384, 1024], P('replica', 'shard')
- new_first: float32 [4, 384, 1024], P('replica', 'shard')
- new_second: float32 [4, 384, 1024], P('replica', 'shard')
The draws below stay inside these ranges and needn't reach their ends.
All inputs are finite; a program needn't handle non-finite values.
Results may differ from the reference program's by a relative error of at most 0.0035.
Values may be sent and summed in bfloat16 or wider, within the bound.
A program may use at most 64 MiB of HBM per device.

```python
import math
import jax
import jax.numpy as jnp
from jax import lax

D = 8192
KV = 1024
DW = 384
TOK = 256
N_REPLICA = 4


def shard_levels(stream_key, dims, split, smallest, high):
    def one(axis_at, parts):
        heights = jax.random.uniform(jax.random.fold_in(jax.random.fold_in(stream_key, 6), axis_at), (parts,), jnp.float32, smallest / len(split), high / len(split))
        return jnp.repeat(jnp.exp(heights), dims[axis_at] // parts).reshape((-1,) + (1,) * (len(dims) - axis_at - 1))

    level = one(*split[0])
    for cut in split[1:]:
        level = level * one(*cut)
    return level


def centred(key, extent, width, reach, shards=(), kind=jnp.bfloat16):
    factor_of = shard_levels(key, extent, shards, -0.22, 0.18) if shards else 1.0
    array = jax.random.normal(key, extent, jnp.float32) * width * factor_of
    return jnp.minimum(jnp.maximum(array, -reach), reach).astype(kind)


def setup_inputs(seed: int = 0) -> dict:
    splits = jax.random.split(jax.random.key(seed), 9)
    return {
        "anchor": centred(splits[0], (DW, D), 1.0, 6.0, ((0, 8),), jnp.float32),
        "replica_rows": centred(splits[1], (N_REPLICA, DW, D), 1.0, 6.0, ((0, 4), (1, 8))),
        "outer_velocity": centred(splits[2], (DW, D), 0.5, 6.0, ((0, 8), (1, 4)), jnp.float32),
        "features": centred(splits[3], (N_REPLICA, DW, TOK), 1.0, 6.0, ((0, 4), (1, 8))),
        "cotangent": centred(splits[4], (N_REPLICA, TOK, KV), TOK ** -0.5, 0.375, ((0, 4), (1, 8))),
        "inner_weight": centred(splits[5], (N_REPLICA, DW, KV), 1.0, 6.0, ((0, 4), (1, 8)), jnp.float32),
        "first_moment": centred(splits[6], (N_REPLICA, DW, KV), 0.5, 6.0, ((0, 4), (1, 8)), jnp.float32),
        "second_moment": jnp.clip(jnp.exp(math.log(2.0) - 1.3862944 * jax.random.uniform(splits[7], (N_REPLICA, DW, KV), jnp.float32) ** shard_levels(splits[7], (N_REPLICA, DW, KV), ((0, 4), (1, 8)), -0.2, 0.2)), 0.5, 2.0),
    }


momentum_keep = 0.9
outer_rate = 0.7
blend_keep = 0.5
inner_rate = 0.01
decay_first = 0.9
decay_second = 0.95
weight_decay = 0.1
epsilon = 1e-08
first_fix = 1.0 - 0.9 ** 10
second_fix = 1.0 - 0.95 ** 10

def reference(anchor, replica_rows, outer_velocity, features, cotangent, inner_weight, first_moment, second_moment):
    drift = anchor[None] - replica_rows.astype(jnp.float32)
    outer_grad = lax.optimization_barrier(jnp.sum(drift, axis=0)) / N_REPLICA
    new_velocity = momentum_keep * outer_velocity + outer_grad
    new_anchor = anchor - outer_rate * (outer_grad + momentum_keep * new_velocity)
    merged_rows = (blend_keep * replica_rows.astype(jnp.float32) + (1.0 - blend_keep) * new_anchor[None]).astype(jnp.bfloat16)
    gradient = jnp.einsum('rdt,rtk->rdk', features.astype(jnp.float32), cotangent.astype(jnp.float32), precision=lax.Precision.HIGHEST)
    new_first = decay_first * first_moment + (1.0 - decay_first) * gradient
    new_second = decay_second * second_moment + (1.0 - decay_second) * gradient * gradient
    stepped = new_first / first_fix / (jnp.sqrt(new_second / second_fix) + epsilon)
    new_weight = inner_weight - inner_rate * (stepped + weight_decay * inner_weight)
    return (new_anchor, merged_rows, new_velocity, new_weight, new_first, new_second)
```

```python
import functools

import jax
import jax.numpy as jnp
from jax import lax
from jax.experimental import pallas as pl
from jax.experimental.pallas import tpu as pltpu
from jax.sharding import PartitionSpec as P

momentum_keep = 0.9
outer_rate = 0.7
blend_keep = 0.5
inner_rate = 0.01
decay_first = 0.9
decay_second = 0.95
weight_decay = 0.1
epsilon = 1e-08
first_fix = 1.0 - 0.9**10
second_fix = 1.0 - 0.95**10

MESH = pl.DeviceIdType.MESH
SPLIT = 4
PARTS = 2
CUTS = 2


def kernel(R, S, anchor_h, rows_h, vel_h, feat_h, cot_h, w_h, m_h, s_h,
           na_o, mg_o, nv_o, nw_o, nm_o, ns_o,
           anchor, rows, vel, feat, cot, wms, sib_rows, msg,
           in_sem, sends, sib_recv, y_recv, own_recv, fwd_recv, z_recv, x_recv,
           ready_y, ready_x, ready_z):
    C, L, H = R // 2, S // 2, SPLIT
    me, at = lax.axis_index("replica"), lax.axis_index("shard")
    y, c = me // 2, me % 2
    pos, x = at // 2, at % 2
    sib = me + 1 - 2 * c
    partner = at + 1 - 2 * x
    W = vel.shape[1]
    piece = W // H
    depth = cot_h.shape[1]
    part_width = cot_h.shape[2] // PARTS

    def columns(q, h):
        return pl.ds(pl.multiple_of(q * W + h * piece, 128), piece)

    def quarter(q):
        return pl.ds(pl.multiple_of(q * W, 128), W)

    def tokens(k):
        return pl.ds(pl.multiple_of(k * depth, depth), depth)

    def block_part(k, u):
        return cot.at[tokens(k), pl.ds(u * part_width, part_width)]

    def tell(semaphore, **target):
        pl.semaphore_signal(semaphore, inc=1, device_id=target, device_id_type=MESH)

    barrier = pltpu.get_barrier_semaphore()
    tell(barrier, replica=sib)
    for t in range(1, C):
        @pl.when(y + t < C)
        def _():
            tell(barrier, replica=me + 2 * t)

    @pl.when(x == 0)
    def _():
        tell(barrier, shard=partner)

    for t in range(1, L):
        @pl.when(pos + t < L)
        def _():
            tell(barrier, shard=at + 2 * t)

    loads = {}

    def load(name, src, dst, slot=None):
        slot = len(loads) if slot is None else slot
        copy = pltpu.make_async_copy(src, dst, in_sem.at[slot])
        copy.start()
        loads[name] = copy

    for j in range(C):
        q = 2 * j + 1 - c
        load(("out", j), rows_h.at[0, :, quarter(q)], rows.at[:, quarter(q)])
    load("cot", cot_h.at[0], cot.at[tokens(at)])
    for j in range(C):
        q = 2 * j + c
        load(("keep", j), rows_h.at[0, :, quarter(q)], rows.at[:, quarter(q)])
    load("anchor", anchor_h, anchor)
    load("vel", vel_h, vel)
    load("feat", feat_h.at[0], feat)
    shared = len(loads)
    for n, source in enumerate((w_h, m_h, s_h)):
        load(("wms", n), source.at[0], wms.at[n], shared)

    pl.semaphore_wait(barrier, 1 + y + x + pos)
    for t in range(1, C):
        @pl.when(y >= t)
        def _():
            tell(ready_y, replica=me - 2 * t)

    @pl.when(x == 1)
    def _():
        tell(ready_x, shard=partner)

    for t in range(1, L):
        @pl.when(pos >= t)
        def _():
            tell(ready_z, shard=at - 2 * t)

    def remote(src, dst, send, recv, **target):
        return pltpu.make_async_remote_copy(
            src_ref=src, dst_ref=dst, send_sem=sends.at[send], recv_sem=recv,
            device_id=target, device_id_type=MESH)

    per = H // CUTS

    def sib_copy(j, g):
        q = 2 * j + 1 - c
        cols = pl.ds(pl.multiple_of(q * W + g * per * piece, 128), per * piece)
        return remote(rows.at[:, cols], sib_rows.at[j, g], 0, sib_recv.at[j, g], replica=sib)

    def cot_copy(k, u, recv, target):
        return remote(block_part(k, u), block_part(k, u), 2, recv, shard=target)

    for j in range(C):
        loads[("out", j)].wait()
        for g in range(CUTS):
            sib_copy(j, g).start()

    loads["cot"].wait()
    for t in range(L - 1, 0, -1):
        @pl.when(pos >= t)
        def _():
            for u in range(PARTS):
                cot_copy(at, u, z_recv.at[t - 1, u], at - 2 * t).start()

    def y_copy(t, j, h):
        return remote(msg.at[c * C + y, j, h], msg.at[c * C + y, j, h], 1,
                      y_recv.at[t - 1, j, h], replica=lax.rem(me + 2 * t, R))

    def own_to_sib(j, h):
        return remote(msg.at[c * C + y, j, h], msg.at[c * C + y, j, h], 1, own_recv, replica=sib)

    def to_sib(t, j, h):
        slot = c * C + lax.rem(y + C - t, C)
        return remote(msg.at[slot, j, h], msg.at[slot, j, h], 1, fwd_recv.at[t - 1, j, h], replica=sib)

    c1 = outer_rate * (1.0 + momentum_keep)
    c2 = outer_rate * momentum_keep * momentum_keep
    share = c1 / R
    for j in range(C):
        loads[("keep", j)].wait()
        if j == 0:
            loads["anchor"].wait()
            loads["vel"].wait()
        mine = y == j
        of_anchor = jnp.where(mine, 0.0, 2.0)
        of_rows = jnp.where(mine, share, -1.0)
        of_vel = jnp.where(mine, -c2, 0.0)
        for h in range(H):
            if h % per == 0:
                sib_copy(j, h // per).wait_recv()
            cols = columns(2 * j + c, h)
            inner = pl.ds(h % per * piece, piece)
            both = rows[:, cols].astype(jnp.float32) + sib_rows[j, h // per, :, inner].astype(jnp.float32)
            value = of_anchor * anchor[:, cols] + of_rows * both
            value = value + of_vel * vel[:, h * piece:(h + 1) * piece]
            msg[c * C + y, j, h] = value.astype(jnp.bfloat16)
            if j == 0 and h == 0:
                @pl.when(y < C - 1)
                def _():
                    pl.semaphore_wait(ready_y, C - 1 - y)

            for t in range(1, C):
                y_copy(t, j, h).start()
            own_to_sib(j, h).start()

    @pl.when(x == 0)
    def _():
        pl.semaphore_wait(ready_x, 1)

    for u in range(PARTS):
        cot_copy(at, u, x_recv, partner).start()

    @pl.when(pos < L - 1)
    def _():
        pl.semaphore_wait(ready_z, L - 1 - pos)

    for t in range(L - 1, 0, -1):
        @pl.when(pos + t < L)
        def _():
            for u in range(PARTS):
                cot_copy(at, u, z_recv.at[L - t - 1, u], at + 2 * t).start()

    def finish(p, j, h):
        cols = columns(2 * j + p, h)
        others = msg[p * C + (j + 1) % C, j, h].astype(jnp.float32)
        for t in range(2, C):
            others = others + msg[p * C + (j + t) % C, j, h].astype(jnp.float32)
        own = msg[p * C + j, j, h].astype(jnp.float32)
        new_anchor = (1.0 - 2.0 * share) * anchor[:, cols] + own - share * others
        na_o[:, cols] = new_anchor
        mg_o[0, :, cols] = (
            blend_keep * rows[:, cols].astype(jnp.float32) + (1.0 - blend_keep) * new_anchor
        ).astype(jnp.bfloat16)

    def finish_velocity(j, h):
        @pl.when(y == j)
        def _():
            cols = columns(2 * j + c, h)
            part = slice(h * piece, (h + 1) * piece)
            inner = pl.ds(h % per * piece, piece)
            total = 2.0 * anchor[:, cols] - (
                rows[:, cols].astype(jnp.float32) + sib_rows[j, h // per, :, inner].astype(jnp.float32))
            for t in range(1, C):
                total = total + msg[c * C + (j + t) % C, j, h].astype(jnp.float32)
            nv_o[:, part] = momentum_keep * vel[:, part] + total / R

    def whole(ref, recv):
        return pltpu.make_async_remote_copy(
            src_ref=ref, dst_ref=ref, send_sem=recv, recv_sem=recv,
            device_id={"replica": sib}, device_id_type=MESH)

    def finish_sib(j, h):
        for t in range(1, C):
            to_sib(t, j, h).wait_recv()
        finish(1 - c, j, h)

    def own_piece(j, h):
        for t in range(1, C):
            y_copy(t, j, h).wait_recv()
            to_sib(t, j, h).start()
        finish(c, j, h)
        finish_velocity(j, h)

    def cot_piece(i, u):
        higher = L - 1 - pos
        d = jnp.where(i < higher, i + 1, L - 1 - (i - higher))
        k = 2 * lax.rem(pos + d, L) + x
        cot_copy(k, u, z_recv.at[d - 1, u], partner).wait_recv()
        cot_copy(k, u, x_recv, partner).start()

    def inner_step():
        whole(cot.at[:L * depth], x_recv).wait_recv()
        loads["feat"].wait()
        pltpu.make_async_copy(wms, wms, in_sem.at[shared]).wait()
        tile = min(256, nw_o.shape[2])
        for n in range(nw_o.shape[2] // tile):
            part = slice(n * tile, (n + 1) * tile)
            gradient = jnp.dot(feat[...], cot[:, part], preferred_element_type=jnp.float32)
            new_first = decay_first * wms[1, :, part] + (1.0 - decay_first) * gradient
            new_second = decay_second * wms[2, :, part] + (1.0 - decay_second) * gradient * gradient
            stepped = new_first / first_fix / (jnp.sqrt(new_second / second_fix) + epsilon)
            weight = wms[0, :, part]
            nw_o[0, :, part] = weight - inner_rate * (stepped + weight_decay * weight)
            nm_o[0, :, part] = new_first
            ns_o[0, :, part] = new_second

    pieces = [(j, h) for j in range(C) for h in range(H)]
    todo = [(i, u) for i in range(L - 1) for u in range(PARTS)]
    each = PARTS * -(-(L - 1) // max(len(pieces) - 5, 1))
    late = len(pieces) - 2
    for i, (j, h) in enumerate(pieces):
        if i == late:
            inner_step()
        own_piece(j, h)
        if i == 1:
            whole(msg.at[0], own_recv).wait_recv()
        if i >= 1:
            finish_sib(*pieces[i - 1])
        for step in todo[i * each:(i + 1) * each]:
            cot_piece(*step)
    finish_sib(*pieces[-1])

    whole(sib_rows, sends.at[0]).wait_send()
    whole(msg.at[:2 * C - 1], sends.at[1]).wait_send()
    whole(cot.at[:(2 * L - 1) * depth], sends.at[2]).wait_send()


def store_kernel(*refs):
    sems = refs[-1]
    count = (len(refs) - 1) // 2
    pairs = list(zip(refs[:count], refs[count:-1]))
    for i, (source, target) in enumerate(pairs):
        rows = source.shape[-2]
        cuts = 3 if rows % 48 == 0 else 1
        for n in range(cuts):
            part = pl.ds(n * (rows // cuts), rows // cuts)
            index = (0, part) if len(source.shape) == 3 else (part,)
            pltpu.make_async_copy(source.at[index], target.at[index], sems.at[i]).start()
    for i, (source, target) in enumerate(pairs):
        pltpu.make_async_copy(source, target, sems.at[i]).wait()


def store(*arrays):
    return pl.pallas_call(
        store_kernel,
        out_shape=tuple(jax.ShapeDtypeStruct(a.shape, a.dtype) for a in arrays),
        in_specs=[pl.BlockSpec(memory_space=pltpu.VMEM)] * len(arrays),
        out_specs=tuple(pl.BlockSpec(memory_space=pltpu.HBM) for _ in arrays),
        scratch_shapes=[pltpu.SemaphoreType.DMA((len(arrays),))],
        compiler_params=pltpu.CompilerParams(vmem_limit_bytes=2**20),
    )(*arrays)


def local(R, S, anchor, replica_rows, outer_velocity, features, cotangent,
          inner_weight, first_moment, second_moment):
    C, L, H = R // 2, S // 2, SPLIT
    height = anchor.shape[0]
    W = outer_velocity.shape[1]
    f32, bf16 = jnp.float32, jnp.bfloat16
    args = (anchor, replica_rows, outer_velocity, features, cotangent,
            inner_weight, first_moment, second_moment)
    outs = (anchor, replica_rows, outer_velocity, inner_weight, first_moment, second_moment)
    dma, regular = pltpu.SemaphoreType.DMA, pltpu.SemaphoreType.REGULAR
    room = 67043328 - sum(a.size * a.dtype.itemsize for a in outs) - 2**16
    results = pl.pallas_call(
        functools.partial(kernel, R, S),
        out_shape=tuple(pltpu.VMEM(a.shape, a.dtype) for a in outs),
        in_specs=[pl.BlockSpec(memory_space=pltpu.HBM)] * len(args),
        out_specs=tuple(pl.BlockSpec(memory_space=pltpu.VMEM) for _ in outs),
        scratch_shapes=[
            pltpu.VMEM(anchor.shape, f32),
            pltpu.VMEM(replica_rows.shape[1:], bf16),
            pltpu.VMEM(outer_velocity.shape, f32),
            pltpu.VMEM(features.shape[1:], bf16),
            pltpu.VMEM((S * cotangent.shape[1], cotangent.shape[2]), bf16),
            pltpu.VMEM((3,) + inner_weight.shape[1:], f32),
            pltpu.VMEM((C, CUTS, height, W // CUTS), bf16),
            pltpu.VMEM((2 * C, C, H, height, W // H), bf16),
            dma((5 + 2 * C,)),
            dma((3,)),
            dma((C, CUTS)),
            dma((C - 1, C, H)),
            dma,
            dma((C - 1, C, H)),
            dma((max(L - 1, 1), PARTS)),
            dma,
            regular,
            regular,
            regular,
        ],
        compiler_params=pltpu.CompilerParams(
            collective_id=0, has_side_effects=True, vmem_limit_bytes=room),
    )(*args)
    return store(*results)


def solution(mesh):
    in_specs = (
        P("shard", None),
        P("replica", "shard", None),
        P("shard", "replica"),
        P("replica", "shard", None),
        P("replica", "shard", None),
        P("replica", "shard", None),
        P("replica", "shard", None),
        P("replica", "shard", None),
    )
    out_specs = (
        P("shard", None),
        P("replica", "shard", None),
        P("shard", "replica"),
        P("replica", "shard", None),
        P("replica", "shard", None),
        P("replica", "shard", None),
    )
    body = functools.partial(local, mesh.shape["replica"], mesh.shape["shard"])
    return jax.shard_map(body, mesh=mesh, in_specs=in_specs, out_specs=out_specs, check_vma=False)
```

```python
import functools

import jax
import jax.numpy as jnp
from jax import lax
from jax.experimental import pallas as pl
from jax.experimental.pallas import tpu as pltpu
from jax.sharding import PartitionSpec as P

momentum_keep = 0.9
outer_rate = 0.7
blend_keep = 0.5
inner_rate = 0.01
decay_first = 0.9
decay_second = 0.95
weight_decay = 0.1
epsilon = 1e-08
first_fix = 1.0 - 0.9**10
second_fix = 1.0 - 0.95**10

MESH = pl.DeviceIdType.MESH
SPLIT = 4
PARTS = 4
CUTS = 2
EXTRA = 1
LAG = 3


def kernel(R, S, anchor_h, rows_h, vel_h, feat_h, cot_h, w_h, m_h, s_h,
           na_o, mg_o, nv_o, nw_o, nm_o, ns_o,
           anchor, rows, vel, feat, cot, wms, sib_rows, more_rows, more_vel, msg,
           in_sem, sends, sib_recv, more_recv, y_recv, more_y, own_recv, fwd_recv, high_fwd, more_fwd,
           z_recv, x_recv, ready_y, ready_x, ready_z):
    C, L, H = R // 2, S // 2, SPLIT
    LOW = H - EXTRA
    me, at = lax.axis_index("replica"), lax.axis_index("shard")
    y, c = me // 2, me % 2
    pos, x = at // 2, at % 2
    sib = me + 1 - 2 * c
    partner = at + 1 - 2 * x
    W = vel.shape[1]
    piece = W // H
    per = H // CUTS
    depth = cot_h.shape[1]
    part_width = cot_h.shape[2] // PARTS
    c1 = outer_rate * (1.0 + momentum_keep)
    c2 = outer_rate * momentum_keep * momentum_keep
    share = c1 / R

    def columns(q, h, count=1):
        return pl.ds(pl.multiple_of(q * W + h * piece, 128), count * piece)

    def quarter(q):
        return columns(q, 0, H)

    def tokens(k):
        return pl.ds(pl.multiple_of(k * depth, depth), depth)

    def turn(r):
        return lax.rem(y + r, C)

    def tell(semaphore, **target):
        pl.semaphore_signal(semaphore, inc=1, device_id=target, device_id_type=MESH)

    barrier = pltpu.get_barrier_semaphore()
    tell(barrier, replica=sib)
    for t in range(1, C):
        @pl.when(y + t < C)
        def _():
            tell(barrier, replica=me + 2 * t)

    @pl.when(x == 0)
    def _():
        tell(barrier, shard=partner)

    for t in range(1, L):
        @pl.when(pos + t < L)
        def _():
            tell(barrier, shard=at + 2 * t)

    OUT, COT, VEL, FEAT, WMS, REST, KEEP = 0, 1, 2, 3, 4, 5, 6
    NEAR = KEEP + C

    def load(src, dst, slot):
        copy = pltpu.make_async_copy(src, dst, in_sem.at[slot])
        copy.start()
        return copy

    for r in range(C):
        cols = quarter(2 * turn(r) + 1 - c)
        load(rows_h.at[0, :, cols], rows.at[:, cols], OUT)
    cot_load = load(cot_h.at[0], cot.at[tokens(at)], COT)
    keep_load, near_load = [], []
    for r in range(C):
        cols = quarter(2 * turn(r) + c)
        keep_load.append(load(rows_h.at[0, :, cols], rows.at[:, cols], KEEP + r))
        if r == 0:
            vel_load = load(vel_h, vel, VEL)
        else:
            near_load.append(load(anchor_h.at[:, cols], anchor.at[:, cols], NEAR + r - 1))

    pl.semaphore_wait(barrier, 1 + y + x + pos)
    for t in range(1, C):
        @pl.when(y >= t)
        def _():
            tell(ready_y, replica=me - 2 * t)

    @pl.when(x == 1)
    def _():
        tell(ready_x, shard=partner)

    for t in range(1, L):
        @pl.when(pos >= t)
        def _():
            tell(ready_z.at[t - 1], shard=at - 2 * t)

    def remote(src, dst, send, recv, **target):
        return pltpu.make_async_remote_copy(
            src_ref=src, dst_ref=dst, send_sem=sends.at[send], recv_sem=recv,
            device_id=target, device_id_type=MESH)

    def whole(ref, semaphore):
        return pltpu.make_async_remote_copy(
            src_ref=ref, dst_ref=ref, send_sem=semaphore, recv_sem=semaphore,
            device_id={"replica": sib}, device_id_type=MESH)

    def sib_copy(j, g):
        cols = columns(2 * j + 1 - c, g * per, per)
        return remote(rows.at[:, cols], sib_rows.at[j, g], 0, sib_recv.at[j, g], replica=sib)

    def more_copy(j):
        cols = columns(2 * j, LOW, EXTRA)
        return remote(rows.at[:, cols], more_rows.at[j], 0, more_recv.at[0], replica=sib)

    def more_vel_copy():
        return remote(vel.at[:, pl.ds(LOW * piece, EXTRA * piece)], more_vel, 0, more_recv.at[1], replica=sib)

    def cot_copy(k, u, recv, target):
        block = cot.at[tokens(k), pl.ds(u * part_width, part_width)]
        return remote(block, block, 2, recv, shard=target)

    def left_sends():
        for t in range(L - 1, 0, -1):
            @pl.when(pos >= t)
            def _():
                for u in range(PARTS):
                    cot_copy(at, u, z_recv.at[t - 1, u], at - 2 * t).start()

    pltpu.make_async_copy(rows_h.at[0, :, pl.ds(0, C * W)], rows.at[:, pl.ds(0, C * W)], in_sem.at[OUT]).wait()
    for r in range(C):
        for g in range(CUTS):
            sib_copy(turn(r), g).start()
    for q in [2 * turn(0) + c] + [2 * turn(r) + 1 - c for r in range(C)]:
        load(anchor_h.at[:, quarter(q)], anchor.at[:, quarter(q)], REST)
    load(feat_h.at[0], feat, FEAT)
    for n, source in enumerate((w_h, m_h, s_h)):
        load(source.at[0], wms.at[n], WMS)
    cot_load.wait()
    pl.when(c == 0)(left_sends)

    def slot(p, src, j, h):
        return ((p * C + src) * C + j) * H + h

    def message(p, src, j, h):
        return msg.at[slot(p, src, j, h)]

    def y_copy(t, p, j, h, recv):
        return remote(message(p, y, j, h), message(p, y, j, h), 1, recv, replica=lax.rem(me + 2 * t, R))

    def own_to_sib(p, j, h):
        return remote(message(p, y, j, h), message(p, y, j, h), 1, own_recv, replica=sib)

    def to_sib(t, p, j, h, recv):
        src = lax.rem(y + C - t, C)
        return remote(message(p, src, j, h), message(p, src, j, h), 1, recv, replica=sib)

    def add_message(p, r, h, other_rows, velocity):
        j = turn(r)
        cols = columns(2 * j + p, h)
        both = rows[:, cols].astype(jnp.float32) + other_rows.astype(jnp.float32)
        if r == 0:
            value = share * both - c2 * velocity
        else:
            value = 2.0 * anchor[:, cols] - both
        msg[slot(p, y, j, h)] = value.astype(jnp.bfloat16)

    def from_sib(j, h):
        return sib_rows[j, h // per, :, pl.ds(h % per * piece, piece)]

    for r in range(C):
        j = turn(r)
        keep_load[r].wait()

        @pl.when(c == 0)
        def _():
            more_copy(j).start()

        if r == 0:
            vel_load.wait()

            @pl.when(c == 0)
            def _():
                more_vel_copy().start()
        else:
            near_load[r - 1].wait()

        for h in range(H):
            if h % per == 0:
                sib_copy(j, h // per).wait_recv()

            def handle():
                add_message(c, r, h, from_sib(j, h), vel[:, h * piece:(h + 1) * piece])
                if r == 0 and h == 0:
                    @pl.when(y < C - 1)
                    def _():
                        pl.semaphore_wait(ready_y, C - 1 - y)

                for t in range(1, C):
                    y_copy(t, c, j, h, y_recv.at[t - 1, r, h]).start()
                own_to_sib(c, j, h).start()

            if h < LOW:
                handle()
            else:
                pl.when(c == 1)(handle)

    pl.when(c == 1)(left_sends)

    @pl.when(x == 0)
    def _():
        pl.semaphore_wait(ready_x, 1)

    for u in range(PARTS):
        cot_copy(at, u, x_recv, partner).start()

    pltpu.make_async_copy(
        anchor_h.at[:, pl.ds(0, (C + 1) * W)], anchor.at[:, pl.ds(0, (C + 1) * W)], in_sem.at[REST]).wait()

    @pl.when(c == 1)
    def _():
        whole(more_rows, more_recv.at[0]).wait_recv()
        more_vel_copy().wait_recv()
        for r in range(C):
            for n in range(EXTRA):
                h, inner = LOW + n, pl.ds(n * piece, piece)
                add_message(0, r, h, more_rows[turn(r), :, inner], more_vel[:, inner])
                for t in range(1, C):
                    y_copy(t, 0, turn(r), h, more_y.at[t - 1, r, n]).start()
                own_to_sib(0, turn(r), h).start()

    for t in range(1, L):
        @pl.when(pos + t < L)
        def _():
            pl.semaphore_wait(ready_z.at[t - 1], 1)
            for u in range(PARTS):
                cot_copy(at, u, z_recv.at[L - t - 1, u], at + 2 * t).start()

    def finish(p, j, h):
        cols = columns(2 * j + p, h)
        others = msg[slot(p, lax.rem(j + 1, C), j, h)].astype(jnp.float32)
        for t in range(2, C):
            others = others + msg[slot(p, lax.rem(j + t, C), j, h)].astype(jnp.float32)
        own = msg[slot(p, j, j, h)].astype(jnp.float32)
        new_anchor = (1.0 - 2.0 * share) * anchor[:, cols] + own - share * others
        na_o[:, cols] = new_anchor
        mg_o[0, :, cols] = (
            blend_keep * rows[:, cols].astype(jnp.float32) + (1.0 - blend_keep) * new_anchor
        ).astype(jnp.bfloat16)

    def finish_velocity(r, h):
        if r == C - 1:
            cols = columns(2 * y + c, h)
            part = slice(h * piece, (h + 1) * piece)
            total = 2.0 * anchor[:, cols] - (
                rows[:, cols].astype(jnp.float32) + from_sib(y, h).astype(jnp.float32))
            for t in range(1, C):
                total = total + msg[slot(c, lax.rem(y + t, C), y, h)].astype(jnp.float32)
            nv_o[:, part] = momentum_keep * vel[:, part] + total / R

    def came(r):
        return turn(r + 1)

    def sent(r, t):
        return (r + 1 + t) % C

    def own_piece(r, h, forward):
        for t in range(1, C):
            y_copy(t, c, came(r), h, y_recv.at[t - 1, sent(r, t), h]).wait_recv()
            to_sib(t, c, came(r), h, forward).start()
        finish(c, came(r), h)
        finish_velocity(r, h)

    def more_piece(r, n):
        for t in range(1, C):
            y_copy(t, 0, came(r), LOW + n, more_y.at[t - 1, sent(r, t), n]).wait_recv()
            to_sib(t, 0, came(r), LOW + n, more_fwd).start()
        finish(0, came(r), LOW + n)

    def pieces_from_sib(n, semaphore):
        whole(msg.at[:n], semaphore).wait_recv()

    def low_group(r):
        pieces_from_sib((C - 1) * LOW, fwd_recv.at[r])
        for h in range(LOW):
            finish(1 - c, came(r), h)

    def cot_piece(i, u):
        higher = L - 1 - pos
        d = jnp.where(i < higher, i + 1, L - 1 - (i - higher))
        k = 2 * lax.rem(pos + d, L) + x
        cot_copy(k, u, z_recv.at[d - 1, u], partner).wait_recv()
        cot_copy(k, u, x_recv, partner).start()

    def inner_step():
        whole(cot.at[:L * depth], x_recv).wait_recv()
        pltpu.make_async_copy(feat_h.at[0], feat, in_sem.at[FEAT]).wait()
        pltpu.make_async_copy(wms, wms, in_sem.at[WMS]).wait()
        tile = min(256, nw_o.shape[2])
        for n in range(nw_o.shape[2] // tile):
            part = slice(n * tile, (n + 1) * tile)
            gradient = jnp.dot(feat[...], cot[:, part], preferred_element_type=jnp.float32)
            new_first = decay_first * wms[1, :, part] + (1.0 - decay_first) * gradient
            new_second = decay_second * wms[2, :, part] + (1.0 - decay_second) * gradient * gradient
            stepped = new_first / first_fix / (jnp.sqrt(new_second / second_fix) + epsilon)
            weight = wms[0, :, part]
            nw_o[0, :, part] = weight - inner_rate * (stepped + weight_decay * weight)
            nm_o[0, :, part] = new_first
            ns_o[0, :, part] = new_second

    low = [(r, h) for r in range(C) for h in range(LOW)]
    todo = [(i, u) for i in range(L - 1) for u in range(PARTS)]
    each = PARTS * -(-(L - 1) // max(len(low) - 2, 1))
    ready = []
    for i, (r, h) in enumerate(low):
        for step in todo[i * each:(i + 1) * each]:
            cot_piece(*step)
        own_piece(r, h, fwd_recv.at[r])
        if i == LAG - 1:
            @pl.when(c == 0)
            def _():
                pieces_from_sib(C * (H + EXTRA), own_recv)

            @pl.when(c == 1)
            def _():
                pieces_from_sib(C * LOW, own_recv)

        if h == LOW - 1:
            ready.append(r)
        if len(ready) > 1 and h == LOW - 2:
            low_group(ready.pop(0))

    @pl.when(c == 1)
    def _():
        for r in range(C):
            for h in range(LOW, H):
                own_piece(r, h, high_fwd)
        for r in ready:
            low_group(r)
        for r in range(C):
            for n in range(EXTRA):
                more_piece(r, n)
        inner_step()

    @pl.when(c == 0)
    def _():
        for r in ready:
            low_group(r)
        pieces_from_sib((C - 1) * C * EXTRA, high_fwd)
        for r in range(C):
            for h in range(LOW, H):
                finish(1, came(r), h)
        inner_step()
        pieces_from_sib((C - 1) * C * EXTRA, more_fwd)
        for r in range(C):
            for h in range(LOW, H):
                finish(0, came(r), h)
                finish_velocity(r, h)

    whole(cot.at[:(2 * L - 1) * depth], sends.at[2]).wait_send()

    @pl.when(c == 0)
    def _():
        whole(rows.at[:, pl.ds(0, (C * (H + EXTRA) + 2 * EXTRA) * piece)], sends.at[0]).wait_send()
        whole(msg.at[:(2 * C - 1) * C * LOW], sends.at[1]).wait_send()

    @pl.when(c == 1)
    def _():
        whole(sib_rows, sends.at[0]).wait_send()
        whole(msg.at[:(2 * C - 1) * C * (H + EXTRA)], sends.at[1]).wait_send()


def store_kernel(*refs):
    sems = refs[-1]
    count = (len(refs) - 1) // 2
    pairs = list(zip(refs[:count], refs[count:-1]))
    for i, (source, target) in enumerate(pairs):
        rows = source.shape[-2]
        cuts = 3 if rows % 48 == 0 else 1
        for n in range(cuts):
            part = pl.ds(n * (rows // cuts), rows // cuts)
            index = (0, part) if len(source.shape) == 3 else (part,)
            pltpu.make_async_copy(source.at[index], target.at[index], sems.at[i]).start()
    for i, (source, target) in enumerate(pairs):
        pltpu.make_async_copy(source, target, sems.at[i]).wait()


def store(*arrays):
    return pl.pallas_call(
        store_kernel,
        out_shape=tuple(jax.ShapeDtypeStruct(a.shape, a.dtype) for a in arrays),
        in_specs=[pl.BlockSpec(memory_space=pltpu.VMEM)] * len(arrays),
        out_specs=tuple(pl.BlockSpec(memory_space=pltpu.HBM) for _ in arrays),
        scratch_shapes=[pltpu.SemaphoreType.DMA((len(arrays),))],
        compiler_params=pltpu.CompilerParams(vmem_limit_bytes=2**20),
    )(*arrays)


def local(R, S, anchor, replica_rows, outer_velocity, features, cotangent,
          inner_weight, first_moment, second_moment):
    C, L, H = R // 2, S // 2, SPLIT
    height = anchor.shape[0]
    W = outer_velocity.shape[1]
    f32, bf16 = jnp.float32, jnp.bfloat16
    args = (anchor, replica_rows, outer_velocity, features, cotangent,
            inner_weight, first_moment, second_moment)
    outs = (anchor, replica_rows, outer_velocity, inner_weight, first_moment, second_moment)
    dma, regular = pltpu.SemaphoreType.DMA, pltpu.SemaphoreType.REGULAR
    room = 67043328 - sum(a.size * a.dtype.itemsize for a in outs) - 2**16
    results = pl.pallas_call(
        functools.partial(kernel, R, S),
        out_shape=tuple(pltpu.VMEM(a.shape, a.dtype) for a in outs),
        in_specs=[pl.BlockSpec(memory_space=pltpu.HBM)] * len(args),
        out_specs=tuple(pl.BlockSpec(memory_space=pltpu.VMEM) for _ in outs),
        scratch_shapes=[
            pltpu.VMEM(anchor.shape, f32),
            pltpu.VMEM(replica_rows.shape[1:], bf16),
            pltpu.VMEM(outer_velocity.shape, f32),
            pltpu.VMEM(features.shape[1:], bf16),
            pltpu.VMEM((S * cotangent.shape[1], cotangent.shape[2]), bf16),
            pltpu.VMEM((3,) + inner_weight.shape[1:], f32),
            pltpu.VMEM((C, CUTS, height, W // CUTS), bf16),
            pltpu.VMEM((C, height, EXTRA * (W // H)), bf16),
            pltpu.VMEM((height, EXTRA * (W // H)), f32),
            pltpu.VMEM((2 * C * C * (H + EXTRA), height, W // H), bf16),
            dma((5 + 2 * C,)),
            dma((3,)),
            dma((C, CUTS)),
            dma((2,)),
            dma((C - 1, C, H)),
            dma((C - 1, C, EXTRA)),
            dma,
            dma((C,)),
            dma,
            dma,
            dma((max(L - 1, 1), PARTS)),
            dma,
            regular,
            regular,
            regular((max(L - 1, 1),)),
        ],
        compiler_params=pltpu.CompilerParams(
            collective_id=0, has_side_effects=True, vmem_limit_bytes=room),
    )(*args)
    return store(*results)


def solution(mesh):
    in_specs = (
        P("shard", None),
        P("replica", "shard", None),
        P("shard", "replica"),
        P("replica", "shard", None),
        P("replica", "shard", None),
        P("replica", "shard", None),
        P("replica", "shard", None),
        P("replica", "shard", None),
    )
    out_specs = (
        P("shard", None),
        P("replica", "shard", None),
        P("shard", "replica"),
        P("replica", "shard", None),
        P("replica", "shard", None),
        P("replica", "shard", None),
    )
    body = functools.partial(local, mesh.shape["replica"], mesh.shape["shard"])
    return jax.shard_map(body, mesh=mesh, in_specs=in_specs, out_specs=out_specs, check_vma=False)
```

```python
import functools

import jax
import jax.numpy as jnp
from jax import lax
from jax.experimental import pallas as pl
from jax.experimental.pallas import tpu as pltpu
from jax.sharding import PartitionSpec as P

momentum_keep = 0.9
outer_rate = 0.7
blend_keep = 0.5
inner_rate = 0.01
decay_first = 0.9
decay_second = 0.95
weight_decay = 0.1
epsilon = 1e-08
first_fix = 1.0 - 0.9**10
second_fix = 1.0 - 0.95**10

MESH = pl.DeviceIdType.MESH
SPLIT = 4
PARTS = 4
CUTS = 2
EXTRA = 1
LAG = 3


def kernel(R, S, anchor_h, rows_h, vel_h, feat_h, cot_h, w_h, m_h, s_h,
           na_o, mg_o, nv_o, nw_o, nm_o, ns_o,
           anchor, rows, vel, feat, cot, wms, sib_rows, more_rows, more_vel, msg,
           in_sem, sends, sib_recv, more_recv, y_recv, more_y, own_recv, fwd_recv, high_fwd, more_fwd,
           z_recv, x_recv, ready_y, ready_x, ready_z):
    C, L, H = R // 2, S // 2, SPLIT
    LOW = H - EXTRA
    me, at = lax.axis_index("replica"), lax.axis_index("shard")
    y, c = me // 2, me % 2
    pos, x = at // 2, at % 2
    sib = me + 1 - 2 * c
    partner = at + 1 - 2 * x
    W = vel.shape[1]
    piece = W // H
    per = H // CUTS
    depth = cot_h.shape[1]
    part_width = cot_h.shape[2] // PARTS
    c1 = outer_rate * (1.0 + momentum_keep)
    c2 = outer_rate * momentum_keep * momentum_keep
    share = c1 / R

    def columns(q, h, count=1):
        return pl.ds(pl.multiple_of(q * W + h * piece, 128), count * piece)

    def quarter(q):
        return columns(q, 0, H)

    def tokens(k):
        return pl.ds(pl.multiple_of(k * depth, depth), depth)

    def turn(r):
        return lax.rem(y + r, C)

    def tell(semaphore, **target):
        pl.semaphore_signal(semaphore, inc=1, device_id=target, device_id_type=MESH)

    barrier = pltpu.get_barrier_semaphore()
    tell(barrier, replica=sib)
    for t in range(1, C):
        @pl.when(y + t < C)
        def _():
            tell(barrier, replica=me + 2 * t)

    @pl.when(x == 0)
    def _():
        tell(barrier, shard=partner)

    for t in range(1, L):
        @pl.when(pos + t < L)
        def _():
            tell(barrier, shard=at + 2 * t)

    FIRST, OUT, COT, VEL, FEAT, WMS, REST, KEEP = range(8)
    NEAR = KEEP + C

    def load(src, dst, slot):
        copy = pltpu.make_async_copy(src, dst, in_sem.at[slot])
        copy.start()
        return copy

    for r in range(C):
        for g in range(CUTS):
            cols = columns(2 * turn(r) + 1 - c, g * per, per)
            load(rows_h.at[0, :, cols], rows.at[:, cols], OUT if r or g else FIRST)
    cot_load = load(cot_h.at[0], cot.at[tokens(at)], COT)
    keep_load, near_load = [], []
    for r in range(C):
        cols = quarter(2 * turn(r) + c)
        keep_load.append(load(rows_h.at[0, :, cols], rows.at[:, cols], KEEP + r))
        if r == 0:
            vel_load = load(vel_h, vel, VEL)
        else:
            near_load.append(load(anchor_h.at[:, cols], anchor.at[:, cols], NEAR + r - 1))

    pl.semaphore_wait(barrier, 1 + y + x + pos)
    for t in range(1, C):
        @pl.when(y >= t)
        def _():
            tell(ready_y, replica=me - 2 * t)

    @pl.when(x == 1)
    def _():
        tell(ready_x, shard=partner)

    for t in range(1, L):
        @pl.when(pos >= t)
        def _():
            tell(ready_z.at[t - 1], shard=at - 2 * t)

    def remote(src, dst, send, recv, **target):
        return pltpu.make_async_remote_copy(
            src_ref=src, dst_ref=dst, send_sem=sends.at[send], recv_sem=recv,
            device_id=target, device_id_type=MESH)

    def whole(ref, semaphore):
        return pltpu.make_async_remote_copy(
            src_ref=ref, dst_ref=ref, send_sem=semaphore, recv_sem=semaphore,
            device_id={"replica": sib}, device_id_type=MESH)

    def sib_copy(j, g):
        cols = columns(2 * j + 1 - c, g * per, per)
        return remote(rows.at[:, cols], sib_rows.at[j, g], 0, sib_recv.at[j, g], replica=sib)

    def more_copy(j):
        cols = columns(2 * j, LOW, EXTRA)
        return remote(rows.at[:, cols], more_rows.at[j], 0, more_recv.at[0], replica=sib)

    def more_vel_copy():
        return remote(vel.at[:, pl.ds(LOW * piece, EXTRA * piece)], more_vel, 0, more_recv.at[1], replica=sib)

    def cot_copy(k, u, recv, target):
        block = cot.at[tokens(k), pl.ds(u * part_width, part_width)]
        return remote(block, block, 2, recv, shard=target)

    def left_sends():
        for t in range(L - 1, 0, -1):
            @pl.when((pos >= 1) if t == 1 else (pos == L - 1))
            def _():
                for u in range(PARTS):
                    cot_copy(at, u, z_recv.at[t - 1, u], at - 2 * t).start()

    def loaded(count, semaphore):
        cols = pl.ds(0, count * piece)
        pltpu.make_async_copy(rows_h.at[0, :, cols], rows.at[:, cols], in_sem.at[semaphore]).wait()

    loaded(per, FIRST)
    sib_copy(turn(0), 0).start()
    loaded(C * H - per, OUT)
    for r in range(C):
        for g in range(CUTS):
            if r or g:
                sib_copy(turn(r), g).start()
    for q in [2 * turn(0) + c] + [2 * turn(r) + 1 - c for r in range(C)]:
        load(anchor_h.at[:, quarter(q)], anchor.at[:, quarter(q)], REST)
    load(feat_h.at[0], feat, FEAT)
    for n, source in enumerate((w_h, m_h, s_h)):
        load(source.at[0], wms.at[n], WMS)
    cot_load.wait()
    pl.when(c == 0)(left_sends)

    def slot(p, src, j, h):
        return ((p * C + src) * C + j) * H + h

    def message(p, src, j, h):
        return msg.at[slot(p, src, j, h)]

    def y_copy(t, p, j, h, recv):
        return remote(message(p, y, j, h), message(p, y, j, h), 1, recv, replica=lax.rem(me + 2 * t, R))

    def own_to_sib(p, j, h):
        return remote(message(p, y, j, h), message(p, y, j, h), 1, own_recv, replica=sib)

    def to_sib(t, p, j, h, recv):
        src = lax.rem(y + C - t, C)
        return remote(message(p, src, j, h), message(p, src, j, h), 1, recv, replica=sib)

    def add_message(p, r, h, other_rows, velocity):
        j = turn(r)
        cols = columns(2 * j + p, h)
        both = rows[:, cols].astype(jnp.float32) + other_rows.astype(jnp.float32)
        if r == 0:
            value = share * both - c2 * velocity
        else:
            value = 2.0 * anchor[:, cols] - both
        msg[slot(p, y, j, h)] = value.astype(jnp.bfloat16)

    def from_sib(j, h):
        return sib_rows[j, h // per, :, pl.ds(h % per * piece, piece)]

    for r in range(C):
        j = turn(r)
        keep_load[r].wait()

        @pl.when(c == 0)
        def _():
            more_copy(j).start()

        if r == 0:
            vel_load.wait()

            @pl.when(c == 0)
            def _():
                more_vel_copy().start()
        else:
            near_load[r - 1].wait()

        for h in range(H):
            if h % per == 0:
                sib_copy(j, h // per).wait_recv()

            def handle():
                add_message(c, r, h, from_sib(j, h), vel[:, h * piece:(h + 1) * piece])
                if r == 0 and h == 0:
                    @pl.when(y < C - 1)
                    def _():
                        pl.semaphore_wait(ready_y, C - 1 - y)

                for t in range(1, C):
                    y_copy(t, c, j, h, y_recv.at[t - 1, r, h]).start()
                own_to_sib(c, j, h).start()

            if h < LOW:
                handle()
            else:
                pl.when(c == 1)(handle)

        if r == 0:
            pl.when(c == 1)(left_sends)

    @pl.when(x == 0)
    def _():
        pl.semaphore_wait(ready_x, 1)

    for u in range(PARTS):
        cot_copy(at, u, x_recv, partner).start()

    pltpu.make_async_copy(
        anchor_h.at[:, pl.ds(0, (C + 1) * W)], anchor.at[:, pl.ds(0, (C + 1) * W)], in_sem.at[REST]).wait()

    @pl.when(c == 1)
    def _():
        whole(more_rows, more_recv.at[0]).wait_recv()
        more_vel_copy().wait_recv()
        for r in range(C):
            for n in range(EXTRA):
                h, inner = LOW + n, pl.ds(n * piece, piece)
                add_message(0, r, h, more_rows[turn(r), :, inner], more_vel[:, inner])
                for t in range(1, C):
                    y_copy(t, 0, turn(r), h, more_y.at[t - 1, r, n]).start()
                own_to_sib(0, turn(r), h).start()

    for t in range(1, L):
        @pl.when(pos + t < L)
        def _():
            pl.semaphore_wait(ready_z.at[t - 1], 1)

        @pl.when((pos + 1 < L) if t == 1 else (pos == 0))
        def _():
            for u in range(PARTS):
                cot_copy(at, u, z_recv.at[L - t - 1, u], at + 2 * t).start()

    def finish(p, j, h):
        cols = columns(2 * j + p, h)
        others = msg[slot(p, lax.rem(j + 1, C), j, h)].astype(jnp.float32)
        for t in range(2, C):
            others = others + msg[slot(p, lax.rem(j + t, C), j, h)].astype(jnp.float32)
        own = msg[slot(p, j, j, h)].astype(jnp.float32)
        new_anchor = (1.0 - 2.0 * share) * anchor[:, cols] + own - share * others
        na_o[:, cols] = new_anchor
        mg_o[0, :, cols] = (
            blend_keep * rows[:, cols].astype(jnp.float32) + (1.0 - blend_keep) * new_anchor
        ).astype(jnp.bfloat16)

    def finish_velocity(r, h):
        if r == C - 1:
            cols = columns(2 * y + c, h)
            part = slice(h * piece, (h + 1) * piece)
            total = 2.0 * anchor[:, cols] - (
                rows[:, cols].astype(jnp.float32) + from_sib(y, h).astype(jnp.float32))
            for t in range(1, C):
                total = total + msg[slot(c, lax.rem(y + t, C), y, h)].astype(jnp.float32)
            nv_o[:, part] = momentum_keep * vel[:, part] + total / R

    def came(r):
        return turn(r + 1)

    def sent(r, t):
        return (r + 1 + t) % C

    def own_piece(r, h, forward):
        for t in range(1, C):
            y_copy(t, c, came(r), h, y_recv.at[t - 1, sent(r, t), h]).wait_recv()
            to_sib(t, c, came(r), h, forward).start()
        finish(c, came(r), h)
        finish_velocity(r, h)

    def more_piece(r, n):
        for t in range(1, C):
            y_copy(t, 0, came(r), LOW + n, more_y.at[t - 1, sent(r, t), n]).wait_recv()
            to_sib(t, 0, came(r), LOW + n, more_fwd).start()
        finish(0, came(r), LOW + n)

    def pieces_from_sib(n, semaphore):
        whole(msg.at[:n], semaphore).wait_recv()

    def low_group(r):
        pieces_from_sib((C - 1) * LOW, fwd_recv.at[r])
        for h in range(LOW):
            finish(1 - c, came(r), h)

    def cot_piece(i, u):
        higher = L - 1 - pos
        source = jnp.where(i < higher, pos + i + 1, pos - 1 - (i - higher))
        if i > 0:
            source = jnp.where(pos == 0, L - 1 if i == 1 else i, source)
            source = jnp.where(pos == L - 1, 0 if i == 1 else L - 1 - i, source)
        d = lax.rem(source - pos + L, L)
        k = 2 * source + x
        cot_copy(k, u, z_recv.at[d - 1, u], partner).wait_recv()
        inner = (source > 0) & (source < L - 1)

        @pl.when(inner & (source > pos) & (pos > 0))
        def _():
            cot_copy(k, u, z_recv.at[d, u], at - 2).start()

        @pl.when(inner & (source < pos) & (pos < L - 1))
        def _():
            cot_copy(k, u, z_recv.at[d - 2, u], at + 2).start()

        cot_copy(k, u, x_recv, partner).start()

    def inner_step():
        whole(cot.at[:L * depth], x_recv).wait_recv()
        pltpu.make_async_copy(feat_h.at[0], feat, in_sem.at[FEAT]).wait()
        pltpu.make_async_copy(wms, wms, in_sem.at[WMS]).wait()
        tile = min(256, nw_o.shape[2])
        for n in range(nw_o.shape[2] // tile):
            part = slice(n * tile, (n + 1) * tile)
            gradient = jnp.dot(feat[...], cot[:, part], preferred_element_type=jnp.float32)
            new_first = decay_first * wms[1, :, part] + (1.0 - decay_first) * gradient
            new_second = decay_second * wms[2, :, part] + (1.0 - decay_second) * gradient * gradient
            stepped = new_first / first_fix / (jnp.sqrt(new_second / second_fix) + epsilon)
            weight = wms[0, :, part]
            nw_o[0, :, part] = weight - inner_rate * (stepped + weight_decay * weight)
            nm_o[0, :, part] = new_first
            ns_o[0, :, part] = new_second

    low = [(r, h) for r in range(C) for h in range(LOW)]
    todo = [(i, u) for i in range(L - 1) for u in range(PARTS)]
    each = PARTS * -(-(L - 1) // max(len(low) - 2, 1))
    ready = []
    for i, (r, h) in enumerate(low):
        for step in todo[i * each:(i + 1) * each]:
            cot_piece(*step)
        own_piece(r, h, fwd_recv.at[r])
        if i == LAG - 1:
            @pl.when(c == 0)
            def _():
                pieces_from_sib(C * (H + EXTRA), own_recv)

            @pl.when(c == 1)
            def _():
                pieces_from_sib(C * LOW, own_recv)

        if h == LOW - 1:
            ready.append(r)
        if len(ready) > 1 and h == LOW - 2:
            low_group(ready.pop(0))

    @pl.when(c == 1)
    def _():
        for r in range(C):
            for h in range(LOW, H):
                own_piece(r, h, high_fwd)
        for r in ready:
            low_group(r)
        for r in range(C):
            for n in range(EXTRA):
                more_piece(r, n)
        inner_step()

    @pl.when(c == 0)
    def _():
        for r in ready:
            low_group(r)
        pieces_from_sib((C - 1) * C * EXTRA, high_fwd)
        for r in range(C):
            for h in range(LOW, H):
                finish(1, came(r), h)
        inner_step()
        pieces_from_sib((C - 1) * C * EXTRA, more_fwd)
        for r in range(C):
            for h in range(LOW, H):
                finish(0, came(r), h)
                finish_velocity(r, h)

    whole(cot.at[:(2 * L - 1) * depth], sends.at[2]).wait_send()

    @pl.when(c == 0)
    def _():
        whole(rows.at[:, pl.ds(0, (C * (H + EXTRA) + 2 * EXTRA) * piece)], sends.at[0]).wait_send()
        whole(msg.at[:(2 * C - 1) * C * LOW], sends.at[1]).wait_send()

    @pl.when(c == 1)
    def _():
        whole(sib_rows, sends.at[0]).wait_send()
        whole(msg.at[:(2 * C - 1) * C * (H + EXTRA)], sends.at[1]).wait_send()


def store_kernel(*refs):
    sems = refs[-1]
    count = (len(refs) - 1) // 2
    pairs = list(zip(refs[:count], refs[count:-1]))
    for i, (source, target) in enumerate(pairs):
        rows = source.shape[-2]
        cuts = 1
        for n in range(cuts):
            part = pl.ds(n * (rows // cuts), rows // cuts)
            index = (0, part) if len(source.shape) == 3 else (part,)
            pltpu.make_async_copy(source.at[index], target.at[index], sems.at[i]).start()
    for i, (source, target) in enumerate(pairs):
        pltpu.make_async_copy(source, target, sems.at[i]).wait()


def store(*arrays):
    return pl.pallas_call(
        store_kernel,
        out_shape=tuple(jax.ShapeDtypeStruct(a.shape, a.dtype) for a in arrays),
        in_specs=[pl.BlockSpec(memory_space=pltpu.VMEM)] * len(arrays),
        out_specs=tuple(pl.BlockSpec(memory_space=pltpu.HBM) for _ in arrays),
        scratch_shapes=[pltpu.SemaphoreType.DMA((len(arrays),))],
        compiler_params=pltpu.CompilerParams(vmem_limit_bytes=2**20),
    )(*arrays)


def local(R, S, anchor, replica_rows, outer_velocity, features, cotangent,
          inner_weight, first_moment, second_moment):
    C, L, H = R // 2, S // 2, SPLIT
    height = anchor.shape[0]
    W = outer_velocity.shape[1]
    f32, bf16 = jnp.float32, jnp.bfloat16
    args = (anchor, replica_rows, outer_velocity, features, cotangent,
            inner_weight, first_moment, second_moment)
    outs = (anchor, replica_rows, outer_velocity, inner_weight, first_moment, second_moment)
    dma, regular = pltpu.SemaphoreType.DMA, pltpu.SemaphoreType.REGULAR
    room = 67043328 - sum(a.size * a.dtype.itemsize for a in outs) - 2**16
    results = pl.pallas_call(
        functools.partial(kernel, R, S),
        out_shape=tuple(pltpu.VMEM(a.shape, a.dtype) for a in outs),
        in_specs=[pl.BlockSpec(memory_space=pltpu.HBM)] * len(args),
        out_specs=tuple(pl.BlockSpec(memory_space=pltpu.VMEM) for _ in outs),
        scratch_shapes=[
            pltpu.VMEM(anchor.shape, f32),
            pltpu.VMEM(replica_rows.shape[1:], bf16),
            pltpu.VMEM(outer_velocity.shape, f32),
            pltpu.VMEM(features.shape[1:], bf16),
            pltpu.VMEM((S * cotangent.shape[1], cotangent.shape[2]), bf16),
            pltpu.VMEM((3,) + inner_weight.shape[1:], f32),
            pltpu.VMEM((C, CUTS, height, W // CUTS), bf16),
            pltpu.VMEM((C, height, EXTRA * (W // H)), bf16),
            pltpu.VMEM((height, EXTRA * (W // H)), f32),
            pltpu.VMEM((2 * C * C * (H + EXTRA), height, W // H), bf16),
            dma((7 + 2 * C,)),
            dma((3,)),
            dma((C, CUTS)),
            dma((2,)),
            dma((C - 1, C, H)),
            dma((C - 1, C, EXTRA)),
            dma,
            dma((C,)),
            dma,
            dma,
            dma((max(L - 1, 1), PARTS)),
            dma,
            regular,
            regular,
            regular((max(L - 1, 1),)),
        ],
        compiler_params=pltpu.CompilerParams(
            collective_id=0, has_side_effects=True, vmem_limit_bytes=room),
    )(*args)
    return store(*results)


def solution(mesh):
    in_specs = (
        P("shard", None),
        P("replica", "shard", None),
        P("shard", "replica"),
        P("replica", "shard", None),
        P("replica", "shard", None),
        P("replica", "shard", None),
        P("replica", "shard", None),
        P("replica", "shard", None),
    )
    out_specs = (
        P("shard", None),
        P("replica", "shard", None),
        P("shard", "replica"),
        P("replica", "shard", None),
        P("replica", "shard", None),
        P("replica", "shard", None),
    )
    body = functools.partial(local, mesh.shape["replica"], mesh.shape["shard"])
    return jax.shard_map(body, mesh=mesh, in_specs=in_specs, out_specs=out_specs, check_vma=False)
```

```python
import functools

import jax
import jax.numpy as jnp
from jax import lax
from jax.experimental import pallas as pl
from jax.experimental.pallas import tpu as pltpu
from jax.sharding import PartitionSpec as P

momentum_keep = 0.9
outer_rate = 0.7
blend_keep = 0.5
inner_rate = 0.01
decay_first = 0.9
decay_second = 0.95
weight_decay = 0.1
epsilon = 1e-08
first_fix = 1.0 - 0.9**10
second_fix = 1.0 - 0.95**10

MESH = pl.DeviceIdType.MESH
SPLIT = 4
PARTS = 4
CUTS = 2
EXTRA = 1


def kernel(R, S, anchor_h, rows_h, vel_h, feat_h, cot_h, w_h, m_h, s_h,
           na_o, mg_o, nv_o, nw_o, nm_o, ns_o,
           anchor, rows, vel, feat, cot, wms, sib_rows, more_rows, more_vel, msg,
           in_sem, sends, sib_recv, more_recv, y_recv, more_y, z_recv, x_recv, ready_y, ready_x, ready_z):
    C, L, H = R // 2, S // 2, SPLIT
    LOW = H - EXTRA
    me, at = lax.axis_index("replica"), lax.axis_index("shard")
    y, c = me // 2, me % 2
    pos, x = at // 2, at % 2
    sib = me + 1 - 2 * c
    partner = at + 1 - 2 * x
    W = vel.shape[1]
    piece = W // H
    per = H // CUTS
    depth = cot_h.shape[1]
    part_width = cot_h.shape[2] // PARTS
    c1 = outer_rate * (1.0 + momentum_keep)
    c2 = outer_rate * momentum_keep * momentum_keep
    share = c1 / R

    def columns(q, h, count=1):
        return pl.ds(pl.multiple_of(q * W + h * piece, 128), count * piece)

    def quarter(q):
        return columns(q, 0, H)

    def tokens(k):
        return pl.ds(pl.multiple_of(k * depth, depth), depth)

    def turn(r):
        return lax.rem(y + r, C)

    def tell(semaphore, **target):
        pl.semaphore_signal(semaphore, inc=1, device_id=target, device_id_type=MESH)

    barrier = pltpu.get_barrier_semaphore()
    tell(barrier, replica=sib)
    for t in range(1, C):
        @pl.when(y + t < C)
        def _():
            tell(barrier, replica=me + 2 * t)

    @pl.when(x == 0)
    def _():
        tell(barrier, shard=partner)

    for t in range(1, L):
        @pl.when(pos + t < L)
        def _():
            tell(barrier, shard=at + 2 * t)

    FIRST, OUT, COT, VEL, INNER, REST, KEEP = range(7)
    NEAR = KEEP + C
    own_recv, high_fwd, more_fwd = in_sem.at[FIRST], in_sem.at[VEL], in_sem.at[COT]

    def load(src, dst, slot):
        copy = pltpu.make_async_copy(src, dst, in_sem.at[slot])
        copy.start()
        return copy

    for r in range(C):
        for g in range(CUTS):
            cols = columns(2 * turn(r) + 1 - c, g * per, per)
            load(rows_h.at[0, :, cols], rows.at[:, cols], OUT if r or g else FIRST)
    cot_load = load(cot_h.at[0], cot.at[tokens(at)], COT)
    keep_load, near_load = [], []
    for r in range(C):
        cols = quarter(2 * turn(r) + c)
        keep_load.append(load(rows_h.at[0, :, cols], rows.at[:, cols], KEEP + r))
        if r == 0:
            vel_load = load(vel_h, vel, VEL)
        else:
            near_load.append(load(anchor_h.at[:, cols], anchor.at[:, cols], NEAR + r - 1))

    pl.semaphore_wait(barrier, 1 + y + x + pos)
    for t in range(1, C):
        @pl.when(y >= t)
        def _():
            tell(ready_y, replica=me - 2 * t)

    @pl.when(x == 1)
    def _():
        tell(ready_x, shard=partner)

    for t in range(1, L):
        @pl.when(pos >= t)
        def _():
            tell(ready_z.at[t - 1], shard=at - 2 * t)

    def remote(src, dst, send, recv, **target):
        return pltpu.make_async_remote_copy(
            src_ref=src, dst_ref=dst, send_sem=sends.at[send], recv_sem=recv,
            device_id=target, device_id_type=MESH)

    def whole(ref, semaphore):
        return pltpu.make_async_remote_copy(
            src_ref=ref, dst_ref=ref, send_sem=semaphore, recv_sem=semaphore,
            device_id={"replica": sib}, device_id_type=MESH)

    def sib_copy(j, g):
        cols = columns(2 * j + 1 - c, g * per, per)
        return remote(rows.at[:, cols], sib_rows.at[j, g], 0, sib_recv.at[j, g], replica=sib)

    def more_copy(j):
        cols = columns(2 * j, LOW, EXTRA)
        return remote(rows.at[:, cols], more_rows.at[j], 0, more_recv.at[0], replica=sib)

    def more_vel_copy():
        return remote(vel.at[:, pl.ds(LOW * piece, EXTRA * piece)], more_vel, 0, more_recv.at[1], replica=sib)

    def cot_copy(k, u, recv, target):
        block = cot.at[tokens(k), pl.ds(u * part_width, part_width)]
        return remote(block, block, 2, recv, shard=target)

    def left_sends():
        for t in range(L - 1, 0, -1):
            @pl.when((pos >= 1) if t == 1 else (pos == L - 1))
            def _():
                for u in range(PARTS):
                    cot_copy(at, u, z_recv.at[t - 1, u], at - 2 * t).start()

    def loaded(count, semaphore):
        cols = pl.ds(0, count * piece)
        pltpu.make_async_copy(rows_h.at[0, :, cols], rows.at[:, cols], in_sem.at[semaphore]).wait()

    loaded(per, FIRST)
    sib_copy(turn(0), 0).start()
    loaded(C * H - per, OUT)
    for r in range(C):
        for g in range(CUTS):
            if r or g:
                sib_copy(turn(r), g).start()
    for q in [2 * turn(0) + c] + [2 * turn(r) + 1 - c for r in range(C)]:
        load(anchor_h.at[:, quarter(q)], anchor.at[:, quarter(q)], REST)
    load(feat_h.at[0], feat, INNER)
    for n, source in enumerate((w_h, m_h, s_h)):
        load(source.at[0], wms.at[n], INNER)
    cot_load.wait()
    pl.when(c == 0)(left_sends)

    def slot(p, src, j, h):
        return ((p * C + src) * C + j) * H + h

    def message(p, src, j, h):
        return msg.at[slot(p, src, j, h)]

    def y_copy(t, p, j, h, recv):
        return remote(message(p, y, j, h), message(p, y, j, h), 1, recv, replica=lax.rem(me + 2 * t, R))

    def own_to_sib(p, j, h):
        return remote(message(p, y, j, h), message(p, y, j, h), 1, own_recv, replica=sib)

    def to_sib(t, p, j, h, recv):
        src = lax.rem(y + C - t, C)
        return remote(message(p, src, j, h), message(p, src, j, h), 1, recv, replica=sib)

    def more_across(t, j, n):
        block = message(0, y, j, LOW + n)
        return remote(block, block, 1, more_y.at[t - 1, C - 1, n], replica=2 * lax.rem(y + t, C))

    def add_message(p, r, h, other_rows, velocity):
        j = turn(r)
        cols = columns(2 * j + p, h)
        both = rows[:, cols].astype(jnp.float32) + other_rows.astype(jnp.float32)
        if r == 0:
            value = share * both - c2 * velocity
        else:
            value = 2.0 * anchor[:, cols] - both
        msg[slot(p, y, j, h)] = value.astype(jnp.bfloat16)

    def from_sib(j, h):
        return sib_rows[j, h // per, :, pl.ds(h % per * piece, piece)]

    for r in range(C):
        j = turn(r)
        keep_load[r].wait()

        @pl.when(c == 0)
        def _():
            more_copy(j).start()

        if r == 0:
            vel_load.wait()

            @pl.when(c == 0)
            def _():
                more_vel_copy().start()
        else:
            near_load[r - 1].wait()

        for h in range(H):
            if h % per == 0:
                sib_copy(j, h // per).wait_recv()

            def handle():
                add_message(c, r, h, from_sib(j, h), vel[:, h * piece:(h + 1) * piece])
                if r == 0 and h == 0:
                    @pl.when(y < C - 1)
                    def _():
                        pl.semaphore_wait(ready_y, C - 1 - y)

                for t in range(1, C):
                    y_copy(t, c, j, h, y_recv.at[t - 1, r, h]).start()
                own_to_sib(c, j, h).start()

            if h < LOW:
                handle()
            else:
                pl.when(c == 1)(handle)

        if r == 0:
            pl.when(c == 1)(left_sends)

    @pl.when(x == 0)
    def _():
        pl.semaphore_wait(ready_x, 1)

    for u in range(PARTS):
        cot_copy(at, u, x_recv, partner).start()

    pltpu.make_async_copy(
        anchor_h.at[:, pl.ds(0, (C + 1) * W)], anchor.at[:, pl.ds(0, (C + 1) * W)], in_sem.at[REST]).wait()

    @pl.when(c == 1)
    def _():
        whole(more_rows, more_recv.at[0]).wait_recv()
        more_vel_copy().wait_recv()
        for r in range(C):
            for n in range(EXTRA):
                h, inner = LOW + n, pl.ds(n * piece, piece)
                add_message(0, r, h, more_rows[turn(r), :, inner], more_vel[:, inner])
                for t in range(1, C):
                    if r == C - 1:
                        more_across(t, turn(r), n).start()
                    y_copy(t, 0, turn(r), h, more_y.at[t - 1, r, n]).start()
                own_to_sib(0, turn(r), h).start()

    for t in range(1, L):
        @pl.when(pos + t < L)
        def _():
            pl.semaphore_wait(ready_z.at[t - 1], 1)

        @pl.when((pos + 1 < L) if t == 1 else (pos == 0))
        def _():
            for u in range(PARTS):
                cot_copy(at, u, z_recv.at[L - t - 1, u], at + 2 * t).start()

    def finish(p, j, h):
        cols = columns(2 * j + p, h)
        others = msg[slot(p, lax.rem(j + 1, C), j, h)].astype(jnp.float32)
        for t in range(2, C):
            others = others + msg[slot(p, lax.rem(j + t, C), j, h)].astype(jnp.float32)
        own = msg[slot(p, j, j, h)].astype(jnp.float32)
        new_anchor = (1.0 - 2.0 * share) * anchor[:, cols] + own - share * others
        na_o[:, cols] = new_anchor
        mg_o[0, :, cols] = (
            blend_keep * rows[:, cols].astype(jnp.float32) + (1.0 - blend_keep) * new_anchor
        ).astype(jnp.bfloat16)

    def finish_velocity(r, h):
        if r == C - 1:
            cols = columns(2 * y + c, h)
            part = slice(h * piece, (h + 1) * piece)
            total = 2.0 * anchor[:, cols] - (
                rows[:, cols].astype(jnp.float32) + from_sib(y, h).astype(jnp.float32))
            for t in range(1, C):
                total = total + msg[slot(c, lax.rem(y + t, C), y, h)].astype(jnp.float32)
            nv_o[:, part] = momentum_keep * vel[:, part] + total / R

    def came(r):
        return turn(r + 1)

    def sent(r, t):
        return (r + 1 + t) % C

    def own_piece(r, h, forward):
        for t in range(1, C):
            y_copy(t, c, came(r), h, y_recv.at[t - 1, sent(r, t), h]).wait_recv()
            to_sib(t, c, came(r), h, forward).start()
        finish(c, came(r), h)
        finish_velocity(r, h)

    def more_piece(r, n):
        for t in range(1, C):
            y_copy(t, 0, came(r), LOW + n, more_y.at[t - 1, sent(r, t), n]).wait_recv()
            if sent(r, t) < C - 1:
                to_sib(t, 0, came(r), LOW + n, more_fwd).start()
        finish(0, came(r), LOW + n)

    def more_own(r, n):
        for t in range(1, C):
            if sent(r, t) == C - 1:
                more_across(t, came(r), n).wait_recv()
        finish(0, came(r), LOW + n)
        finish_velocity(r, LOW + n)

    def pieces_from_sib(n, semaphore):
        whole(msg.at[:n], semaphore).wait_recv()

    def low_group(r):
        pieces_from_sib((C - 1) * LOW, in_sem.at[KEEP + r])
        for h in range(LOW):
            finish(1 - c, came(r), h)

    def cot_piece(i, u):
        higher = L - 1 - pos
        source = jnp.where(i < higher, pos + i + 1, pos - 1 - (i - higher))
        if i > 0:
            source = jnp.where(pos == 0, L - 1 if i == 1 else i, source)
            source = jnp.where(pos == L - 1, 0 if i == 1 else L - 1 - i, source)
        d = lax.rem(source - pos + L, L)
        k = 2 * source + x
        cot_copy(k, u, z_recv.at[d - 1, u], partner).wait_recv()
        inner = (source > 0) & (source < L - 1)

        @pl.when(inner & (source > pos) & (pos > 0))
        def _():
            cot_copy(k, u, z_recv.at[d, u], at - 2).start()

        @pl.when(inner & (source < pos) & (pos < L - 1))
        def _():
            cot_copy(k, u, z_recv.at[d - 2, u], at + 2).start()

        cot_copy(k, u, x_recv, partner).start()

    def inner_step():
        whole(cot.at[:L * depth], x_recv).wait_recv()
        cols = pl.ds(0, 3 * wms.shape[2] + feat.shape[1] // 2)
        pltpu.make_async_copy(anchor_h.at[:, cols], anchor.at[:, cols], in_sem.at[INNER]).wait()
        tile = min(256, nw_o.shape[2])
        for n in range(nw_o.shape[2] // tile):
            part = slice(n * tile, (n + 1) * tile)
            gradient = jnp.dot(feat[...], cot[:, part], preferred_element_type=jnp.float32)
            new_first = decay_first * wms[1, :, part] + (1.0 - decay_first) * gradient
            new_second = decay_second * wms[2, :, part] + (1.0 - decay_second) * gradient * gradient
            stepped = new_first / first_fix / (jnp.sqrt(new_second / second_fix) + epsilon)
            weight = wms[0, :, part]
            nw_o[0, :, part] = weight - inner_rate * (stepped + weight_decay * weight)
            nm_o[0, :, part] = new_first
            ns_o[0, :, part] = new_second

    low = [(r, h) for r in range(C) for h in range(LOW)]
    todo = [(i, u) for i in range(L - 1) for u in range(PARTS)]
    each = PARTS * -(-(L - 1) // max(len(low) - 2, 1))
    ready = []
    for i, (r, h) in enumerate(low):
        for step in todo[i * each:(i + 1) * each]:
            cot_piece(*step)
        if i == 0:
            @pl.when(c == 0)
            def _():
                pieces_from_sib(C * (H + EXTRA), own_recv)

            @pl.when(c == 1)
            def _():
                pieces_from_sib(C * LOW, own_recv)

        own_piece(r, h, in_sem.at[KEEP + r])
        if h == LOW - 1:
            ready.append(r)
        if len(ready) > 1 and h == LOW - 2:
            low_group(ready.pop(0))

    @pl.when(c == 1)
    def _():
        for r in range(C):
            for h in range(LOW, H):
                own_piece(r, h, high_fwd)
        for r in ready:
            low_group(r)
        for r in range(C - 1):
            for n in range(EXTRA):
                more_piece(r, n)
        inner_step()
        for n in range(EXTRA):
            more_piece(C - 1, n)

    @pl.when(c == 0)
    def _():
        for r in ready:
            low_group(r)
        pieces_from_sib((C - 1) * C * EXTRA, high_fwd)
        for r in range(C):
            for h in range(LOW, H):
                finish(1, came(r), h)
        inner_step()
        pieces_from_sib((C - 1) * (C - 1) * EXTRA, more_fwd)
        for r in range(C):
            for n in range(EXTRA):
                more_own(r, n)

    whole(cot.at[:(2 * L - 1) * depth], sends.at[2]).wait_send()

    @pl.when(c == 0)
    def _():
        whole(rows.at[:, pl.ds(0, (C * (H + EXTRA) + 2 * EXTRA) * piece)], sends.at[0]).wait_send()
        whole(msg.at[:(2 * C - 1) * C * LOW], sends.at[1]).wait_send()

    @pl.when(c == 1)
    def _():
        whole(sib_rows, sends.at[0]).wait_send()
        whole(msg.at[:(2 * C - 1) * C * (H + EXTRA)], sends.at[1]).wait_send()


def store_kernel(*refs):
    sems = refs[-1]
    count = (len(refs) - 1) // 2
    pairs = list(zip(refs[:count], refs[count:-1]))
    for i, (source, target) in enumerate(pairs):
        rows = source.shape[-2]
        cuts = 1
        for n in range(cuts):
            part = pl.ds(n * (rows // cuts), rows // cuts)
            index = (0, part) if len(source.shape) == 3 else (part,)
            pltpu.make_async_copy(source.at[index], target.at[index], sems.at[i]).start()
    for i, (source, target) in enumerate(pairs):
        pltpu.make_async_copy(source, target, sems.at[i]).wait()


def store(*arrays):
    return pl.pallas_call(
        store_kernel,
        out_shape=tuple(jax.ShapeDtypeStruct(a.shape, a.dtype) for a in arrays),
        in_specs=[pl.BlockSpec(memory_space=pltpu.VMEM)] * len(arrays),
        out_specs=tuple(pl.BlockSpec(memory_space=pltpu.HBM) for _ in arrays),
        scratch_shapes=[pltpu.SemaphoreType.DMA((len(arrays),))],
        compiler_params=pltpu.CompilerParams(vmem_limit_bytes=2**20),
    )(*arrays)


def local(R, S, anchor, replica_rows, outer_velocity, features, cotangent,
          inner_weight, first_moment, second_moment):
    C, L, H = R // 2, S // 2, SPLIT
    height = anchor.shape[0]
    W = outer_velocity.shape[1]
    f32, bf16 = jnp.float32, jnp.bfloat16
    args = (anchor, replica_rows, outer_velocity, features, cotangent,
            inner_weight, first_moment, second_moment)
    outs = (anchor, replica_rows, outer_velocity, inner_weight, first_moment, second_moment)
    dma, regular = pltpu.SemaphoreType.DMA, pltpu.SemaphoreType.REGULAR
    room = 67043328 - sum(a.size * a.dtype.itemsize for a in outs) - 2**16
    results = pl.pallas_call(
        functools.partial(kernel, R, S),
        out_shape=tuple(pltpu.VMEM(a.shape, a.dtype) for a in outs),
        in_specs=[pl.BlockSpec(memory_space=pltpu.HBM)] * len(args),
        out_specs=tuple(pl.BlockSpec(memory_space=pltpu.VMEM) for _ in outs),
        scratch_shapes=[
            pltpu.VMEM(anchor.shape, f32),
            pltpu.VMEM(replica_rows.shape[1:], bf16),
            pltpu.VMEM(outer_velocity.shape, f32),
            pltpu.VMEM(features.shape[1:], bf16),
            pltpu.VMEM((S * cotangent.shape[1], cotangent.shape[2]), bf16),
            pltpu.VMEM((3,) + inner_weight.shape[1:], f32),
            pltpu.VMEM((C, CUTS, height, W // CUTS), bf16),
            pltpu.VMEM((C, height, EXTRA * (W // H)), bf16),
            pltpu.VMEM((height, EXTRA * (W // H)), f32),
            pltpu.VMEM((2 * C * C * (H + EXTRA), height, W // H), bf16),
            dma((6 + 2 * C,)),
            dma((3,)),
            dma((C, CUTS)),
            dma((2,)),
            dma((C - 1, C, H)),
            dma((C - 1, C, EXTRA)),
            dma((max(L - 1, 1), PARTS)),
            dma,
            regular,
            regular,
            regular((max(L - 1, 1),)),
        ],
        compiler_params=pltpu.CompilerParams(
            collective_id=0, has_side_effects=True, vmem_limit_bytes=room),
    )(*args)
    return store(*results)


def solution(mesh):
    in_specs = (
        P("shard", None),
        P("replica", "shard", None),
        P("shard", "replica"),
        P("replica", "shard", None),
        P("replica", "shard", None),
        P("replica", "shard", None),
        P("replica", "shard", None),
        P("replica", "shard", None),
    )
    out_specs = (
        P("shard", None),
        P("replica", "shard", None),
        P("shard", "replica"),
        P("replica", "shard", None),
        P("replica", "shard", None),
        P("replica", "shard", None),
    )
    body = functools.partial(local, mesh.shape["replica"], mesh.shape["shard"])
    return jax.shard_map(body, mesh=mesh, in_specs=in_specs, out_specs=out_specs, check_vma=False)
```

```python
import functools

import jax
import jax.numpy as jnp
from jax import lax
from jax.experimental import pallas as pl
from jax.experimental.pallas import tpu as pltpu
from jax.sharding import PartitionSpec as P

momentum_keep = 0.9
outer_rate = 0.7
blend_keep = 0.5
inner_rate = 0.01
decay_first = 0.9
decay_second = 0.95
weight_decay = 0.1
epsilon = 1e-08
first_fix = 1.0 - 0.9**10
second_fix = 1.0 - 0.95**10

MESH = pl.DeviceIdType.MESH
SPLIT = 4
PARTS = 4
CUTS = 2
EXTRA = 1


def kernel(R, S, anchor_h, rows_h, vel_h, feat_h, cot_h, w_h, m_h, s_h,
           na_o, mg_o, nv_o, nw_o, nm_o, ns_o,
           anchor, rows, vel, feat, cot, wms, sib_rows, more_rows, more_vel, msg,
           in_sem, sends, sib_recv, more_recv, y_recv, more_y, z_recv, x_recv, ready_y, ready_x, ready_z):
    C, L, H = R // 2, S // 2, SPLIT
    LOW = H - EXTRA
    me, at = lax.axis_index("replica"), lax.axis_index("shard")
    y, c = me // 2, me % 2
    pos, x = at // 2, at % 2
    sib = me + 1 - 2 * c
    partner = at + 1 - 2 * x
    W = vel.shape[1]
    piece = W // H
    per = H // CUTS
    depth = cot_h.shape[1]
    part_width = cot_h.shape[2] // PARTS
    c1 = outer_rate * (1.0 + momentum_keep)
    c2 = outer_rate * momentum_keep * momentum_keep
    share = c1 / R

    def columns(q, h, count=1):
        return pl.ds(pl.multiple_of(q * W + h * piece, 128), count * piece)

    def quarter(q):
        return columns(q, 0, H)

    def tokens(k):
        return pl.ds(pl.multiple_of(k * depth, depth), depth)

    def turn(r):
        return lax.rem(y + r, C)

    def tell(semaphore, **target):
        pl.semaphore_signal(semaphore, inc=1, device_id=target, device_id_type=MESH)

    FIRST, COT, INNER, REST, KEEP, OUT = range(6)
    NEAR = OUT + 1
    own_recv, high_fwd, more_fwd = in_sem.at[FIRST], in_sem.at[KEEP], in_sem.at[COT]

    def load(src, dst, slot):
        copy = pltpu.make_async_copy(src, dst, in_sem.at[slot])
        copy.start()
        return copy

    first_cols = columns(2 * turn(0) + 1 - c, 0, per)
    load(rows_h.at[0, :, first_cols], rows.at[:, first_cols], FIRST)

    barrier = pltpu.get_barrier_semaphore()
    tell(barrier, replica=sib)
    for t in range(1, C):
        @pl.when(y + t < C)
        def _():
            tell(barrier, replica=me + 2 * t)

    @pl.when(x == 0)
    def _():
        tell(barrier, shard=partner)

    for t in range(1, L):
        @pl.when(pos + t < L)
        def _():
            tell(barrier, shard=at + 2 * t)

    for r in range(C):
        for g in range(CUTS):
            if r or g:
                cols = columns(2 * turn(r) + 1 - c, g * per, per)
                load(rows_h.at[0, :, cols], rows.at[:, cols], OUT)
    cot_load = load(cot_h.at[0], cot.at[tokens(at)], COT)
    near_load = []
    for r in range(C):
        cols = quarter(2 * turn(r) + c)
        load(rows_h.at[0, :, cols], rows.at[:, cols], KEEP)
        if r == 0:
            load(vel_h, vel, KEEP)
        else:
            near_load.append(load(anchor_h.at[:, cols], anchor.at[:, cols], NEAR + r - 1))

    pl.semaphore_wait(barrier, 1 + y + x + pos)
    for t in range(1, C):
        @pl.when(y >= t)
        def _():
            tell(ready_y, replica=me - 2 * t)

    @pl.when(x == 1)
    def _():
        tell(ready_x, shard=partner)

    for t in range(1, L):
        @pl.when(pos >= t)
        def _():
            tell(ready_z.at[min(t, 2) - 1], shard=at - 2 * t)

    def remote(src, dst, send, recv, **target):
        return pltpu.make_async_remote_copy(
            src_ref=src, dst_ref=dst, send_sem=sends.at[send], recv_sem=recv,
            device_id=target, device_id_type=MESH)

    def whole(ref, semaphore):
        return pltpu.make_async_remote_copy(
            src_ref=ref, dst_ref=ref, send_sem=semaphore, recv_sem=semaphore,
            device_id={"replica": sib}, device_id_type=MESH)

    def sib_copy(j, g):
        cols = columns(2 * j + 1 - c, g * per, per)
        return remote(rows.at[:, cols], sib_rows.at[j, g], 0, sib_recv.at[j, g], replica=sib)

    def more_copy(j):
        cols = columns(2 * j, LOW, EXTRA)
        return remote(rows.at[:, cols], more_rows.at[j], 0, more_recv, replica=sib)

    def more_vel_copy():
        return remote(vel.at[:, pl.ds(LOW * piece, EXTRA * piece)], more_vel, 0, more_recv, replica=sib)

    def cot_copy(k, u, recv, target):
        block = cot.at[tokens(k), pl.ds(u * part_width, part_width)]
        return remote(block, block, 2, recv, shard=target)

    def left_sends():
        for t in range(L - 1, 0, -1):
            @pl.when((pos >= 1) if t == 1 else (pos == L - 1))
            def _():
                for u in range(PARTS):
                    cot_copy(at, u, z_recv.at[t - 1, u], at - 2 * t).start()

    def loaded(count, semaphore):
        cols = pl.ds(0, count * piece)
        pltpu.make_async_copy(rows_h.at[0, :, cols], rows.at[:, cols], in_sem.at[semaphore]).wait()

    loaded(per, FIRST)
    sib_copy(turn(0), 0).start()
    loaded(C * H - per, OUT)
    for r in range(C):
        for g in range(CUTS):
            if r or g:
                sib_copy(turn(r), g).start()
    for q in [2 * turn(0) + c] + [2 * turn(r) + 1 - c for r in range(C)]:
        load(anchor_h.at[:, quarter(q)], anchor.at[:, quarter(q)], REST)
    load(feat_h.at[0], feat, INNER)
    for n, source in enumerate((w_h, m_h, s_h)):
        load(source.at[0], wms.at[n], INNER)
    cot_load.wait()
    pl.when((c == 0) | (pos < L - 1))(left_sends)

    def slot(p, src, j, h):
        return ((p * C + src) * C + j) * H + h

    def message(p, src, j, h):
        return msg.at[slot(p, src, j, h)]

    def y_copy(t, p, j, h, recv):
        return remote(message(p, y, j, h), message(p, y, j, h), 1, recv, replica=lax.rem(me + 2 * t, R))

    def own_to_sib(p, j, h):
        return remote(message(p, y, j, h), message(p, y, j, h), 1, own_recv, replica=sib)

    def to_sib(t, p, j, h, recv):
        src = lax.rem(y + C - t, C)
        return remote(message(p, src, j, h), message(p, src, j, h), 1, recv, replica=sib)

    def more_across(t, j, n):
        block = message(0, y, j, LOW + n)
        return remote(block, block, 1, more_y.at[t - 1, C - 1, n], replica=2 * lax.rem(y + t, C))

    def add_message(p, r, h, other_rows, velocity):
        j = turn(r)
        cols = columns(2 * j + p, h)
        both = rows[:, cols].astype(jnp.float32) + other_rows.astype(jnp.float32)
        if r == 0:
            value = share * both - c2 * velocity
        else:
            value = 2.0 * anchor[:, cols] - both
        msg[slot(p, y, j, h)] = value.astype(jnp.bfloat16)

    def from_sib(j, h):
        return sib_rows[j, h // per, :, pl.ds(h % per * piece, piece)]

    halves = pl.ds(0, C * W // 2 + W)
    pltpu.make_async_copy(anchor_h.at[:, halves], anchor.at[:, halves], in_sem.at[KEEP]).wait()
    for r in range(C):
        j = turn(r)

        @pl.when(c == 0)
        def _():
            more_copy(j).start()

        if r == 0:
            @pl.when(c == 0)
            def _():
                more_vel_copy().start()
        else:
            near_load[r - 1].wait()

        for h in range(H):
            if h % per == 0:
                sib_copy(j, h // per).wait_recv()

            def handle():
                add_message(c, r, h, from_sib(j, h), vel[:, h * piece:(h + 1) * piece])
                if r == 0 and h == 0:
                    @pl.when(y < C - 1)
                    def _():
                        pl.semaphore_wait(ready_y, C - 1 - y)

                for t in range(1, C):
                    y_copy(t, c, j, h, y_recv.at[t - 1, r, h]).start()
                own_to_sib(c, j, h).start()

            if h < LOW:
                handle()
            else:
                pl.when(c == 1)(handle)

        if r == 0:
            pl.when((c == 1) & (pos == L - 1))(left_sends)

    @pl.when(x == 0)
    def _():
        pl.semaphore_wait(ready_x, 1)

    for u in range(PARTS):
        cot_copy(at, u, x_recv, partner).start()

    pltpu.make_async_copy(
        anchor_h.at[:, pl.ds(0, (C + 1) * W)], anchor.at[:, pl.ds(0, (C + 1) * W)], in_sem.at[REST]).wait()

    @pl.when(c == 1)
    def _():
        whole(rows.at[:, pl.ds(0, (C + 2) * EXTRA * piece)], more_recv).wait_recv()
        for r in range(C):
            for n in range(EXTRA):
                h, inner = LOW + n, pl.ds(n * piece, piece)
                add_message(0, r, h, more_rows[turn(r), :, inner], more_vel[:, inner])
                for t in range(1, C):
                    if r == C - 1:
                        more_across(t, turn(r), n).start()
                    y_copy(t, 0, turn(r), h, more_y.at[t - 1, r, n]).start()
                own_to_sib(0, turn(r), h).start()

    @pl.when(pos + 1 < L)
    def _():
        pl.semaphore_wait(ready_z.at[0], 1)
        for u in range(PARTS):
            cot_copy(at, u, z_recv.at[L - 2, u], at + 2).start()

    @pl.when(pos + 2 < L)
    def _():
        pl.semaphore_wait(ready_z.at[1], L - 2 - pos)

    @pl.when(pos == 0)
    def _():
        for t in range(2, L):
            for u in range(PARTS):
                cot_copy(at, u, z_recv.at[L - t - 1, u], at + 2 * t).start()

    def finish(p, j, h):
        cols = columns(2 * j + p, h)
        others = msg[slot(p, lax.rem(j + 1, C), j, h)].astype(jnp.float32)
        for t in range(2, C):
            others = others + msg[slot(p, lax.rem(j + t, C), j, h)].astype(jnp.float32)
        own = msg[slot(p, j, j, h)].astype(jnp.float32)
        new_anchor = (1.0 - 2.0 * share) * anchor[:, cols] + own - share * others
        na_o[:, cols] = new_anchor
        mg_o[0, :, cols] = (
            blend_keep * rows[:, cols].astype(jnp.float32) + (1.0 - blend_keep) * new_anchor
        ).astype(jnp.bfloat16)

    def finish_velocity(r, h):
        if r == C - 1:
            cols = columns(2 * y + c, h)
            part = slice(h * piece, (h + 1) * piece)
            total = 2.0 * anchor[:, cols] - (
                rows[:, cols].astype(jnp.float32) + from_sib(y, h).astype(jnp.float32))
            for t in range(1, C):
                total = total + msg[slot(c, lax.rem(y + t, C), y, h)].astype(jnp.float32)
            nv_o[:, part] = momentum_keep * vel[:, part] + total / R

    def came(r):
        return turn(r + 1)

    def sent(r, t):
        return (r + 1 + t) % C

    def own_piece(r, h, forward):
        for t in range(1, C):
            y_copy(t, c, came(r), h, y_recv.at[t - 1, sent(r, t), h]).wait_recv()
            to_sib(t, c, came(r), h, forward).start()
        finish(c, came(r), h)
        finish_velocity(r, h)

    def more_piece(r, n):
        for t in range(1, C):
            y_copy(t, 0, came(r), LOW + n, more_y.at[t - 1, sent(r, t), n]).wait_recv()
            if sent(r, t) < C - 1:
                to_sib(t, 0, came(r), LOW + n, more_fwd).start()
        finish(0, came(r), LOW + n)

    def more_own(r, n):
        for t in range(1, C):
            if sent(r, t) == C - 1:
                more_across(t, came(r), n).wait_recv()
        finish(0, came(r), LOW + n)
        finish_velocity(r, LOW + n)

    def pieces_from_sib(n, semaphore):
        whole(msg.at[:n], semaphore).wait_recv()

    def low_group(r):
        pieces_from_sib((C - 1) * LOW, in_sem.at[OUT + r])
        for h in range(LOW):
            finish(1 - c, came(r), h)

    def cot_piece(i, u):
        higher = L - 1 - pos
        source = jnp.where(i < higher, pos + i + 1, pos - 1 - (i - higher))
        source = jnp.where(pos == L - 2, pos - 1 - i if i < L - 2 else L - 1, source)
        if i > 0:
            source = jnp.where(pos == 0, L - 1 if i == 1 else i, source)
            source = jnp.where(pos == L - 1, 0 if i == 1 else L - 1 - i, source)
        d = lax.rem(source - pos + L, L)
        k = 2 * source + x
        cot_copy(k, u, z_recv.at[d - 1, u], partner).wait_recv()
        inner = (source > 0) & (source < L - 1)

        @pl.when(inner & (source > pos) & (pos > 0))
        def _():
            cot_copy(k, u, z_recv.at[d, u], at - 2).start()

        @pl.when(inner & (source < pos) & (pos < L - 1))
        def _():
            cot_copy(k, u, z_recv.at[d - 2, u], at + 2).start()

        cot_copy(k, u, x_recv, partner).start()

    def inner_step():
        whole(cot.at[:L * depth], x_recv).wait_recv()
        cols = pl.ds(0, 3 * wms.shape[2] + feat.shape[1] // 2)
        pltpu.make_async_copy(anchor_h.at[:, cols], anchor.at[:, cols], in_sem.at[INNER]).wait()
        tile = min(256, nw_o.shape[2])
        for n in range(nw_o.shape[2] // tile):
            part = slice(n * tile, (n + 1) * tile)
            gradient = jnp.dot(feat[...], cot[:, part], preferred_element_type=jnp.float32)
            new_first = decay_first * wms[1, :, part] + (1.0 - decay_first) * gradient
            new_second = decay_second * wms[2, :, part] + (1.0 - decay_second) * gradient * gradient
            stepped = new_first / first_fix / (jnp.sqrt(new_second / second_fix) + epsilon)
            weight = wms[0, :, part]
            nw_o[0, :, part] = weight - inner_rate * (stepped + weight_decay * weight)
            nm_o[0, :, part] = new_first
            ns_o[0, :, part] = new_second

    low = [(r, h) for r in range(C) for h in range(LOW)]
    todo = [(i, u) for i in range(L - 1) for u in range(PARTS)]
    each = PARTS * -(-(L - 1) // max(len(low) - 2, 1))
    ready = []
    for i, (r, h) in enumerate(low):
        for step in todo[i * each:(i + 1) * each]:
            cot_piece(*step)
        if i == 0:
            @pl.when(c == 0)
            def _():
                pieces_from_sib(C * (H + EXTRA), own_recv)

            @pl.when(c == 1)
            def _():
                pieces_from_sib(C * LOW, own_recv)

        own_piece(r, h, in_sem.at[OUT + r])
        if h == LOW - 1:
            ready.append(r)
        if len(ready) > 1 and h == LOW - 2:
            low_group(ready.pop(0))

    @pl.when(c == 1)
    def _():
        for r in range(C):
            for h in range(LOW, H):
                own_piece(r, h, high_fwd)
        for r in ready:
            low_group(r)
        for r in range(C - 1):
            for n in range(EXTRA):
                more_piece(r, n)
        inner_step()
        for n in range(EXTRA):
            more_piece(C - 1, n)

    @pl.when(c == 0)
    def _():
        for r in ready:
            low_group(r)
        inner_step()
        pieces_from_sib((C - 1) * C * EXTRA, high_fwd)
        for r in range(C):
            for h in range(LOW, H):
                finish(1, came(r), h)
        pieces_from_sib((C - 1) * (C - 1) * EXTRA, more_fwd)
        for r in range(C):
            for n in range(EXTRA):
                more_own(r, n)

    whole(cot.at[:(2 * L - 1) * depth], sends.at[2]).wait_send()

    @pl.when(c == 0)
    def _():
        whole(rows.at[:, pl.ds(0, (C * (H + EXTRA) + 2 * EXTRA) * piece)], sends.at[0]).wait_send()
        whole(msg.at[:(2 * C - 1) * C * LOW], sends.at[1]).wait_send()

    @pl.when(c == 1)
    def _():
        whole(sib_rows, sends.at[0]).wait_send()
        whole(msg.at[:(2 * C - 1) * C * (H + EXTRA)], sends.at[1]).wait_send()


def store_kernel(*refs):
    sems = refs[-1]
    count = (len(refs) - 1) // 2
    pairs = list(zip(refs[:count], refs[count:-1]))
    for i, (source, target) in enumerate(pairs):
        rows = source.shape[-2]
        cuts = 1
        for n in range(cuts):
            part = pl.ds(n * (rows // cuts), rows // cuts)
            index = (0, part) if len(source.shape) == 3 else (part,)
            pltpu.make_async_copy(source.at[index], target.at[index], sems.at[i]).start()
    for i, (source, target) in enumerate(pairs):
        pltpu.make_async_copy(source, target, sems.at[i]).wait()


def store(*arrays):
    return pl.pallas_call(
        store_kernel,
        out_shape=tuple(jax.ShapeDtypeStruct(a.shape, a.dtype) for a in arrays),
        in_specs=[pl.BlockSpec(memory_space=pltpu.VMEM)] * len(arrays),
        out_specs=tuple(pl.BlockSpec(memory_space=pltpu.HBM) for _ in arrays),
        scratch_shapes=[pltpu.SemaphoreType.DMA((len(arrays),))],
        compiler_params=pltpu.CompilerParams(vmem_limit_bytes=2**20),
    )(*arrays)


def local(R, S, anchor, replica_rows, outer_velocity, features, cotangent,
          inner_weight, first_moment, second_moment):
    C, L, H = R // 2, S // 2, SPLIT
    height = anchor.shape[0]
    W = outer_velocity.shape[1]
    f32, bf16 = jnp.float32, jnp.bfloat16
    args = (anchor, replica_rows, outer_velocity, features, cotangent,
            inner_weight, first_moment, second_moment)
    outs = (anchor, replica_rows, outer_velocity, inner_weight, first_moment, second_moment)
    dma, regular = pltpu.SemaphoreType.DMA, pltpu.SemaphoreType.REGULAR
    room = 67043328 - sum(a.size * a.dtype.itemsize for a in outs) - 2**16
    results = pl.pallas_call(
        functools.partial(kernel, R, S),
        out_shape=tuple(pltpu.VMEM(a.shape, a.dtype) for a in outs),
        in_specs=[pl.BlockSpec(memory_space=pltpu.HBM)] * len(args),
        out_specs=tuple(pl.BlockSpec(memory_space=pltpu.VMEM) for _ in outs),
        scratch_shapes=[
            pltpu.VMEM(anchor.shape, f32),
            pltpu.VMEM(replica_rows.shape[1:], bf16),
            pltpu.VMEM(outer_velocity.shape, f32),
            pltpu.VMEM(features.shape[1:], bf16),
            pltpu.VMEM((S * cotangent.shape[1], cotangent.shape[2]), bf16),
            pltpu.VMEM((3,) + inner_weight.shape[1:], f32),
            pltpu.VMEM((C, CUTS, height, W // CUTS), bf16),
            pltpu.VMEM((C, height, EXTRA * (W // H)), bf16),
            pltpu.VMEM((height, EXTRA * (W // H)), f32),
            pltpu.VMEM((2 * C * C * (H + EXTRA), height, W // H), bf16),
            dma((5 + C,)),
            dma((3,)),
            dma((C, CUTS)),
            dma,
            dma((C - 1, C, H)),
            dma((C - 1, C, EXTRA)),
            dma((max(L - 1, 1), PARTS)),
            dma,
            regular,
            regular,
            regular((2,)),
        ],
        compiler_params=pltpu.CompilerParams(
            collective_id=0, has_side_effects=True, vmem_limit_bytes=room),
    )(*args)
    return store(*results)


def solution(mesh):
    in_specs = (
        P("shard", None),
        P("replica", "shard", None),
        P("shard", "replica"),
        P("replica", "shard", None),
        P("replica", "shard", None),
        P("replica", "shard", None),
        P("replica", "shard", None),
        P("replica", "shard", None),
    )
    out_specs = (
        P("shard", None),
        P("replica", "shard", None),
        P("shard", "replica"),
        P("replica", "shard", None),
        P("replica", "shard", None),
        P("replica", "shard", None),
    )
    body = functools.partial(local, mesh.shape["replica"], mesh.shape["shard"])
    return jax.shard_map(body, mesh=mesh, in_specs=in_specs, out_specs=out_specs, check_vma=False)
```

```python
import functools

import jax
import jax.numpy as jnp
from jax import lax
from jax.experimental import pallas as pl
from jax.experimental.pallas import tpu as pltpu
from jax.sharding import PartitionSpec as P

momentum_keep = 0.9
outer_rate = 0.7
blend_keep = 0.5
inner_rate = 0.01
decay_first = 0.9
decay_second = 0.95
weight_decay = 0.1
epsilon = 1e-08
first_fix = 1.0 - 0.9**10
second_fix = 1.0 - 0.95**10

MESH = pl.DeviceIdType.MESH
SPLIT = 4
PARTS = 4
CUTS = 2
EXTRA = 1


def kernel(R, S, anchor_h, rows_h, vel_h, feat_h, cot_h, w_h, m_h, s_h,
           na_o, mg_o, nv_o, nw_o, nm_o, ns_o,
           anchor, rows, vel, feat, cot, wms, sib_rows, more_rows, more_vel, msg, passing,
           in_sem, sends, sib_recv, more_recv, y_recv, more_y, pass_recv, z_recv, x_recv, ready_y, ready_x, ready_z):
    C, L, H = R // 2, S // 2, SPLIT
    LOW = H - EXTRA
    me, at = lax.axis_index("replica"), lax.axis_index("shard")
    y, c = me // 2, me % 2
    pos, x = at // 2, at % 2
    sib = me + 1 - 2 * c
    partner = at + 1 - 2 * x
    W = vel.shape[1]
    piece = W // H
    per = H // CUTS
    depth = cot_h.shape[1]
    part_width = cot_h.shape[2] // PARTS
    c1 = outer_rate * (1.0 + momentum_keep)
    c2 = outer_rate * momentum_keep * momentum_keep
    share = c1 / R

    def columns(q, h, count=1):
        return pl.ds(pl.multiple_of(q * W + h * piece, 128), count * piece)

    def quarter(q):
        return columns(q, 0, H)

    def tokens(k):
        return pl.ds(pl.multiple_of(k * depth, depth), depth)

    def turn(r):
        return lax.rem(y + r, C)

    def tell(semaphore, **target):
        pl.semaphore_signal(semaphore, inc=1, device_id=target, device_id_type=MESH)

    FIRST, COT, INNER, REST, KEEP, OUT = range(6)
    NEAR = OUT + 1
    own_recv, high_fwd, more_fwd = in_sem.at[FIRST], in_sem.at[KEEP], in_sem.at[COT]

    def load(src, dst, slot):
        copy = pltpu.make_async_copy(src, dst, in_sem.at[slot])
        copy.start()
        return copy

    first_cols = columns(2 * turn(0) + 1 - c, 0, per)
    load(rows_h.at[0, :, first_cols], rows.at[:, first_cols], FIRST)

    barrier = pltpu.get_barrier_semaphore()
    tell(barrier, replica=sib)
    for t in range(1, C):
        @pl.when(y + t < C)
        def _():
            tell(barrier, replica=me + 2 * t)

    @pl.when(x == 0)
    def _():
        tell(barrier, shard=partner)

    for t in range(1, L):
        @pl.when(pos + t < L)
        def _():
            tell(barrier, shard=at + 2 * t)

    for r in range(C):
        for g in range(CUTS):
            if r or g:
                cols = columns(2 * turn(r) + 1 - c, g * per, per)
                load(rows_h.at[0, :, cols], rows.at[:, cols], OUT)
    cot_load = load(cot_h.at[0], cot.at[tokens(at)], COT)
    near_load = []
    for r in range(C):
        cols = quarter(2 * turn(r) + c)
        load(rows_h.at[0, :, cols], rows.at[:, cols], KEEP)
        if r == 0:
            load(vel_h, vel, KEEP)
        else:
            near_load.append(load(anchor_h.at[:, cols], anchor.at[:, cols], NEAR + r - 1))

    pl.semaphore_wait(barrier, 1 + y + x + pos)
    for t in range(1, C):
        @pl.when(y >= t)
        def _():
            tell(ready_y, replica=me - 2 * t)

    @pl.when(x == 1)
    def _():
        tell(ready_x, shard=partner)

    for t in range(1, L):
        @pl.when(pos >= t)
        def _():
            tell(ready_z.at[min(t, 2) - 1], shard=at - 2 * t)

    def remote(src, dst, send, recv, **target):
        return pltpu.make_async_remote_copy(
            src_ref=src, dst_ref=dst, send_sem=sends.at[send], recv_sem=recv,
            device_id=target, device_id_type=MESH)

    def whole(ref, semaphore):
        return pltpu.make_async_remote_copy(
            src_ref=ref, dst_ref=ref, send_sem=semaphore, recv_sem=semaphore,
            device_id={"replica": sib}, device_id_type=MESH)

    def sib_copy(j, g):
        cols = columns(2 * j + 1 - c, g * per, per)
        return remote(rows.at[:, cols], sib_rows.at[j, g], 0, sib_recv.at[j, g], replica=sib)

    def more_copy(j):
        cols = columns(2 * j, LOW, EXTRA)
        return remote(rows.at[:, cols], more_rows.at[j], 0, more_recv, replica=sib)

    def more_vel_copy():
        return remote(vel.at[:, pl.ds(LOW * piece, EXTRA * piece)], more_vel, 0, more_recv, replica=sib)

    def cot_copy(k, u, recv, target):
        block = cot.at[tokens(k), pl.ds(u * part_width, part_width)]
        return remote(block, block, 2, recv, shard=target)

    def left_sends():
        for t in range(L - 1, 0, -1):
            @pl.when((pos >= 1) if t == 1 else (pos == L - 1))
            def _():
                for u in range(PARTS):
                    cot_copy(at, u, z_recv.at[t - 1, u], at - 2 * t).start()

    def loaded(count, semaphore):
        cols = pl.ds(0, count * piece)
        pltpu.make_async_copy(rows_h.at[0, :, cols], rows.at[:, cols], in_sem.at[semaphore]).wait()

    loaded(per, FIRST)
    sib_copy(turn(0), 0).start()
    loaded(C * H - per, OUT)
    for r in range(C):
        for g in range(CUTS):
            if r or g:
                sib_copy(turn(r), g).start()
    for q in [2 * turn(0) + c] + [2 * turn(r) + 1 - c for r in range(C)]:
        load(anchor_h.at[:, quarter(q)], anchor.at[:, quarter(q)], REST)
    load(feat_h.at[0], feat, INNER)
    for n, source in enumerate((w_h, m_h, s_h)):
        load(source.at[0], wms.at[n], INNER)
    cot_load.wait()
    pl.when((c == 0) | (pos < L - 1))(left_sends)

    def slot(p, src, j, h):
        return ((p * C + src) * C + j) * H + h

    def message(p, src, j, h):
        return msg.at[slot(p, src, j, h)]

    def y_copy(t, p, j, h, recv):
        return remote(message(p, y, j, h), message(p, y, j, h), 1, recv, replica=lax.rem(me + 2 * t, R))

    def own_to_sib(p, j, h):
        return remote(message(p, y, j, h), message(p, y, j, h), 1, own_recv, replica=sib)

    def to_sib(t, p, j, h, recv):
        src = lax.rem(y + C - t, C)
        return remote(message(p, src, j, h), message(p, src, j, h), 1, recv, replica=sib)

    def more_across(t, j, n):
        block = message(0, y, j, LOW + n)
        return remote(block, block, 1, more_y.at[t - 1, C - 1, n], replica=2 * lax.rem(y + t, C))

    def add_message(p, r, h, other_rows, velocity):
        j = turn(r)
        cols = columns(2 * j + p, h)
        both = rows[:, cols].astype(jnp.float32) + other_rows.astype(jnp.float32)
        if r == 0:
            value = share * both - c2 * velocity
        else:
            value = 2.0 * anchor[:, cols] - both
        msg[slot(p, y, j, h)] = value.astype(jnp.bfloat16)

    goes_around = (y == 1) & (x == 0)
    passes_on = (c == 1) & (y == 0) & (x == 1)

    def around(r, h):
        return C == 2 and r == 0 and h == H - 1

    def pass_copy():
        return remote(passing, message(1, 1, 1, H - 1), 3,
                      y_recv.at[0, 0, H - 1], shard=partner)

    def from_sib(j, h):
        return sib_rows[j, h // per, :, pl.ds(h % per * piece, piece)]

    halves = pl.ds(0, C * W // 2 + W)
    pltpu.make_async_copy(anchor_h.at[:, halves], anchor.at[:, halves], in_sem.at[KEEP]).wait()
    for r in range(C):
        j = turn(r)

        @pl.when(c == 0)
        def _():
            more_copy(j).start()

        if r == 0:
            @pl.when(c == 0)
            def _():
                more_vel_copy().start()
        else:
            near_load[r - 1].wait()

        for h in range(H):
            if h % per == 0:
                sib_copy(j, h // per).wait_recv()

            def handle():
                add_message(c, r, h, from_sib(j, h), vel[:, h * piece:(h + 1) * piece])
                if r == 0 and h == 0:
                    @pl.when(y < C - 1)
                    def _():
                        pl.semaphore_wait(ready_y, C - 1 - y)

                for t in range(1, C):
                    if not around(r, h):
                        y_copy(t, c, j, h, y_recv.at[t - 1, r, h]).start()
                if around(r, h):
                    @pl.when((c == 1) & (x == 0))
                    def _():
                        pl.semaphore_wait(ready_x, 1)

                    @pl.when(goes_around)
                    def _():
                        block = message(1, y, j, h)
                        pltpu.make_async_remote_copy(
                            src_ref=block, dst_ref=passing, send_sem=sends.at[1], recv_sem=pass_recv,
                            device_id=(me - 2, partner), device_id_type=MESH).start()

                    @pl.when(jnp.logical_not(goes_around))
                    def _():
                        y_copy(1, c, j, h, y_recv.at[0, r, h]).start()

                own_to_sib(c, j, h).start()

            if h < LOW:
                handle()
            else:
                pl.when(c == 1)(handle)

    @pl.when((x == 0) if C != 2 else (c == 0) & (x == 0))
    def _():
        pl.semaphore_wait(ready_x, 1)

    pl.when((c == 1) & (pos == L - 1))(left_sends)
    for u in range(PARTS):
        cot_copy(at, u, x_recv, partner).start()

    pltpu.make_async_copy(
        anchor_h.at[:, pl.ds(0, (C + 1) * W)], anchor.at[:, pl.ds(0, (C + 1) * W)], in_sem.at[REST]).wait()

    @pl.when(c == 1)
    def _():
        whole(rows.at[:, pl.ds(0, (C + 2) * EXTRA * piece)], more_recv).wait_recv()
        for r in range(C):
            for n in range(EXTRA):
                h, inner = LOW + n, pl.ds(n * piece, piece)
                add_message(0, r, h, more_rows[turn(r), :, inner], more_vel[:, inner])
                for t in range(1, C):
                    if r == C - 1:
                        more_across(t, turn(r), n).start()
                    y_copy(t, 0, turn(r), h, more_y.at[t - 1, r, n]).start()
                own_to_sib(0, turn(r), h).start()

    @pl.when(pos + 1 < L)
    def _():
        pl.semaphore_wait(ready_z.at[0], 1)
        for u in range(PARTS):
            cot_copy(at, u, z_recv.at[L - 2, u], at + 2).start()

    @pl.when(pos + 2 < L)
    def _():
        pl.semaphore_wait(ready_z.at[1], L - 2 - pos)

    @pl.when(pos == 0)
    def _():
        for t in range(2, L):
            for u in range(PARTS):
                cot_copy(at, u, z_recv.at[L - t - 1, u], at + 2 * t).start()

    def finish(p, j, h):
        cols = columns(2 * j + p, h)
        others = msg[slot(p, lax.rem(j + 1, C), j, h)].astype(jnp.float32)
        for t in range(2, C):
            others = others + msg[slot(p, lax.rem(j + t, C), j, h)].astype(jnp.float32)
        own = msg[slot(p, j, j, h)].astype(jnp.float32)
        new_anchor = (1.0 - 2.0 * share) * anchor[:, cols] + own - share * others
        na_o[:, cols] = new_anchor
        mg_o[0, :, cols] = (
            blend_keep * rows[:, cols].astype(jnp.float32) + (1.0 - blend_keep) * new_anchor
        ).astype(jnp.bfloat16)

    def finish_velocity(r, h):
        if r == C - 1:
            cols = columns(2 * y + c, h)
            part = slice(h * piece, (h + 1) * piece)
            total = 2.0 * anchor[:, cols] - (
                rows[:, cols].astype(jnp.float32) + from_sib(y, h).astype(jnp.float32))
            for t in range(1, C):
                total = total + msg[slot(c, lax.rem(y + t, C), y, h)].astype(jnp.float32)
            nv_o[:, part] = momentum_keep * vel[:, part] + total / R

    def came(r):
        return turn(r + 1)

    def sent(r, t):
        return (r + 1 + t) % C

    def own_piece(r, h, forward):
        for t in range(1, C):
            y_copy(t, c, came(r), h, y_recv.at[t - 1, sent(r, t), h]).wait_recv()
            to_sib(t, c, came(r), h, forward).start()
        finish(c, came(r), h)
        finish_velocity(r, h)

    def more_piece(r, n):
        for t in range(1, C):
            y_copy(t, 0, came(r), LOW + n, more_y.at[t - 1, sent(r, t), n]).wait_recv()
            if sent(r, t) < C - 1:
                to_sib(t, 0, came(r), LOW + n, more_fwd).start()
        finish(0, came(r), LOW + n)

    def more_own(r, n):
        for t in range(1, C):
            if sent(r, t) == C - 1:
                more_across(t, came(r), n).wait_recv()
        finish(0, came(r), LOW + n)
        finish_velocity(r, LOW + n)

    def pieces_from_sib(n, semaphore):
        whole(msg.at[:n], semaphore).wait_recv()

    def low_group(r):
        pieces_from_sib((C - 1) * LOW, in_sem.at[OUT + r])
        for h in range(LOW):
            finish(1 - c, came(r), h)

    def cot_piece(i, u):
        higher = L - 1 - pos
        source = jnp.where(i < higher, pos + i + 1, pos - 1 - (i - higher))
        source = jnp.where(pos == L - 2, pos - 1 - i if i < L - 2 else L - 1, source)
        if i > 0:
            source = jnp.where(pos == 0, L - 1 if i == 1 else i, source)
            source = jnp.where(pos == L - 1, 0 if i == 1 else L - 1 - i, source)
        d = lax.rem(source - pos + L, L)
        k = 2 * source + x
        cot_copy(k, u, z_recv.at[d - 1, u], partner).wait_recv()
        inner = (source > 0) & (source < L - 1)

        @pl.when(inner & (source > pos) & (pos > 0))
        def _():
            cot_copy(k, u, z_recv.at[d, u], at - 2).start()

        @pl.when(inner & (source < pos) & (pos < L - 1))
        def _():
            cot_copy(k, u, z_recv.at[d - 2, u], at + 2).start()

        cot_copy(k, u, x_recv, partner).start()

    def inner_step():
        whole(cot.at[:L * depth], x_recv).wait_recv()
        cols = pl.ds(0, 3 * wms.shape[2] + feat.shape[1] // 2)
        pltpu.make_async_copy(anchor_h.at[:, cols], anchor.at[:, cols], in_sem.at[INNER]).wait()
        tile = min(256, nw_o.shape[2])
        for n in range(nw_o.shape[2] // tile):
            part = slice(n * tile, (n + 1) * tile)
            gradient = jnp.dot(feat[...], cot[:, part], preferred_element_type=jnp.float32)
            new_first = decay_first * wms[1, :, part] + (1.0 - decay_first) * gradient
            new_second = decay_second * wms[2, :, part] + (1.0 - decay_second) * gradient * gradient
            stepped = new_first / first_fix / (jnp.sqrt(new_second / second_fix) + epsilon)
            weight = wms[0, :, part]
            nw_o[0, :, part] = weight - inner_rate * (stepped + weight_decay * weight)
            nm_o[0, :, part] = new_first
            ns_o[0, :, part] = new_second

    low = [(r, h) for r in range(C) for h in range(LOW)]
    todo = [(i, u) for i in range(L - 1) for u in range(PARTS)]
    each = PARTS * -(-(L - 1) // max(len(low) - 2, 1))
    ready = []
    for i, (r, h) in enumerate(low):
        for step in todo[i * each:(i + 1) * each]:
            cot_piece(*step)
        if i == 0:
            @pl.when(c == 0)
            def _():
                pieces_from_sib(C * (H + EXTRA), own_recv)

            @pl.when(c == 1)
            def _():
                pieces_from_sib(C * LOW, own_recv)

        own_piece(r, h, in_sem.at[OUT + r])
        if C == 2 and i == 0:
            @pl.when(passes_on)
            def _():
                whole(passing, pass_recv).wait_recv()
                pass_copy().start()

        if h == LOW - 1:
            ready.append(r)
        if len(ready) > 1 and h == LOW - 2:
            low_group(ready.pop(0))

    @pl.when(c == 1)
    def _():
        for r in range(C):
            for h in range(LOW, H):
                own_piece(r, h, high_fwd)
        for r in range(C - 1):
            for n in range(EXTRA):
                more_piece(r, n)
        for r in ready:
            low_group(r)
        inner_step()
        for n in range(EXTRA):
            more_piece(C - 1, n)

    @pl.when(c == 0)
    def _():
        for r in ready:
            low_group(r)
        inner_step()
        pieces_from_sib((C - 1) * C * EXTRA, high_fwd)
        for r in range(C):
            for h in range(LOW, H):
                finish(1, came(r), h)
        pieces_from_sib((C - 1) * (C - 1) * EXTRA, more_fwd)
        for r in range(C):
            for n in range(EXTRA):
                more_own(r, n)

    whole(cot.at[:(2 * L - 1) * depth], sends.at[2]).wait_send()

    if C == 2:
        @pl.when(passes_on)
        def _():
            pass_copy().wait_send()

    @pl.when(c == 0)
    def _():
        whole(rows.at[:, pl.ds(0, (C * (H + EXTRA) + 2 * EXTRA) * piece)], sends.at[0]).wait_send()
        whole(msg.at[:(2 * C - 1) * C * LOW], sends.at[1]).wait_send()

    @pl.when(c == 1)
    def _():
        whole(sib_rows, sends.at[0]).wait_send()
        whole(msg.at[:(2 * C - 1) * C * (H + EXTRA)], sends.at[1]).wait_send()


def store_kernel(*refs):
    sems = refs[-1]
    count = (len(refs) - 1) // 2
    pairs = list(zip(refs[:count], refs[count:-1]))
    for i, (source, target) in enumerate(pairs):
        rows = source.shape[-2]
        cuts = 1
        for n in range(cuts):
            part = pl.ds(n * (rows // cuts), rows // cuts)
            index = (0, part) if len(source.shape) == 3 else (part,)
            pltpu.make_async_copy(source.at[index], target.at[index], sems.at[i]).start()
    for i, (source, target) in enumerate(pairs):
        pltpu.make_async_copy(source, target, sems.at[i]).wait()


def store(*arrays):
    return pl.pallas_call(
        store_kernel,
        out_shape=tuple(jax.ShapeDtypeStruct(a.shape, a.dtype) for a in arrays),
        in_specs=[pl.BlockSpec(memory_space=pltpu.VMEM)] * len(arrays),
        out_specs=tuple(pl.BlockSpec(memory_space=pltpu.HBM) for _ in arrays),
        scratch_shapes=[pltpu.SemaphoreType.DMA((len(arrays),))],
        compiler_params=pltpu.CompilerParams(vmem_limit_bytes=2**20),
    )(*arrays)


def local(R, S, anchor, replica_rows, outer_velocity, features, cotangent,
          inner_weight, first_moment, second_moment):
    C, L, H = R // 2, S // 2, SPLIT
    height = anchor.shape[0]
    W = outer_velocity.shape[1]
    f32, bf16 = jnp.float32, jnp.bfloat16
    args = (anchor, replica_rows, outer_velocity, features, cotangent,
            inner_weight, first_moment, second_moment)
    outs = (anchor, replica_rows, outer_velocity, inner_weight, first_moment, second_moment)
    dma, regular = pltpu.SemaphoreType.DMA, pltpu.SemaphoreType.REGULAR
    room = 67043328 - sum(a.size * a.dtype.itemsize for a in outs) - 2**16
    results = pl.pallas_call(
        functools.partial(kernel, R, S),
        out_shape=tuple(pltpu.VMEM(a.shape, a.dtype) for a in outs),
        in_specs=[pl.BlockSpec(memory_space=pltpu.HBM)] * len(args),
        out_specs=tuple(pl.BlockSpec(memory_space=pltpu.VMEM) for _ in outs),
        scratch_shapes=[
            pltpu.VMEM(anchor.shape, f32),
            pltpu.VMEM(replica_rows.shape[1:], bf16),
            pltpu.VMEM(outer_velocity.shape, f32),
            pltpu.VMEM(features.shape[1:], bf16),
            pltpu.VMEM((S * cotangent.shape[1], cotangent.shape[2]), bf16),
            pltpu.VMEM((3,) + inner_weight.shape[1:], f32),
            pltpu.VMEM((C, CUTS, height, W // CUTS), bf16),
            pltpu.VMEM((C, height, EXTRA * (W // H)), bf16),
            pltpu.VMEM((height, EXTRA * (W // H)), f32),
            pltpu.VMEM((2 * C * C * (H + EXTRA), height, W // H), bf16),
            pltpu.VMEM((height, W // H), bf16),
            dma((5 + C,)),
            dma((4,)),
            dma((C, CUTS)),
            dma,
            dma((C - 1, C, H)),
            dma((C - 1, C, EXTRA)),
            dma,
            dma((max(L - 1, 1), PARTS)),
            dma,
            regular,
            regular,
            regular((2,)),
        ],
        compiler_params=pltpu.CompilerParams(
            collective_id=0, has_side_effects=True, vmem_limit_bytes=room),
    )(*args)
    return store(*results)


def solution(mesh):
    in_specs = (
        P("shard", None),
        P("replica", "shard", None),
        P("shard", "replica"),
        P("replica", "shard", None),
        P("replica", "shard", None),
        P("replica", "shard", None),
        P("replica", "shard", None),
        P("replica", "shard", None),
    )
    out_specs = (
        P("shard", None),
        P("replica", "shard", None),
        P("shard", "replica"),
        P("replica", "shard", None),
        P("replica", "shard", None),
        P("replica", "shard", None),
    )
    body = functools.partial(local, mesh.shape["replica"], mesh.shape["shard"])
    return jax.shard_map(body, mesh=mesh, in_specs=in_specs, out_specs=out_specs, check_vma=False)
```

```python
import functools

import jax
import jax.numpy as jnp
from jax import lax
from jax.experimental import pallas as pl
from jax.experimental.pallas import tpu as pltpu
from jax.sharding import PartitionSpec as P

momentum_keep = 0.9
outer_rate = 0.7
blend_keep = 0.5
inner_rate = 0.01
decay_first = 0.9
decay_second = 0.95
weight_decay = 0.1
epsilon = 1e-08
first_fix = 1.0 - 0.9**10
second_fix = 1.0 - 0.95**10

MESH = pl.DeviceIdType.MESH
SPLIT = 4
PARTS = 4
CUTS = 2
EXTRA = 1


def kernel(R, S, anchor_h, rows_h, vel_h, feat_h, cot_h, w_h, m_h, s_h,
           na_o, mg_o, nv_o, nw_o, nm_o, ns_o,
           anchor, rows, vel, feat, cot, wms, sib_rows, more_rows, more_vel, msg, passing,
           in_sem, sends, sib_recv, more_recv, y_recv, more_y, pass_recv, z_recv, x_recv, ready_y, ready_x, ready_z):
    C, L, H = R // 2, S // 2, SPLIT
    LOW = H - EXTRA
    me, at = lax.axis_index("replica"), lax.axis_index("shard")
    y, c = me // 2, me % 2
    pos, x = at // 2, at % 2
    sib = me + 1 - 2 * c
    partner = at + 1 - 2 * x
    W = vel.shape[1]
    piece = W // H
    per = H // CUTS
    depth = cot_h.shape[1]
    part_width = cot_h.shape[2] // PARTS
    c1 = outer_rate * (1.0 + momentum_keep)
    c2 = outer_rate * momentum_keep * momentum_keep
    share = c1 / R

    def columns(q, h, count=1):
        return pl.ds(pl.multiple_of(q * W + h * piece, 128), count * piece)

    def quarter(q):
        return columns(q, 0, H)

    def tokens(k):
        return pl.ds(pl.multiple_of(k * depth, depth), depth)

    def turn(r):
        return lax.rem(y + r, C)

    def tell(semaphore, **target):
        pl.semaphore_signal(semaphore, inc=1, device_id=target, device_id_type=MESH)

    FIRST, COT, INNER, REST, KEEP, OUT = range(6)
    NEAR = OUT + 1
    own_recv, high_fwd, more_fwd = in_sem.at[FIRST], in_sem.at[KEEP], in_sem.at[COT]

    def load(src, dst, slot):
        copy = pltpu.make_async_copy(src, dst, in_sem.at[slot])
        copy.start()
        return copy

    first_cols = columns(2 * turn(0) + 1 - c, 0, per)
    load(rows_h.at[0, :, first_cols], rows.at[:, first_cols], FIRST)

    barrier = pltpu.get_barrier_semaphore()
    tell(barrier, replica=sib)
    for t in range(1, C):
        @pl.when(y + t < C)
        def _():
            tell(barrier, replica=me + 2 * t)

    @pl.when(x == 0)
    def _():
        tell(barrier, shard=partner)

    for t in range(1, L):
        @pl.when(pos + t < L)
        def _():
            tell(barrier, shard=at + 2 * t)

    for r in range(C):
        for g in range(CUTS):
            if r or g:
                cols = columns(2 * turn(r) + 1 - c, g * per, per)
                load(rows_h.at[0, :, cols], rows.at[:, cols], OUT)
    cot_load = load(cot_h.at[0], cot.at[tokens(at)], COT)
    near_load = []
    for r in range(C):
        cols = quarter(2 * turn(r) + c)
        load(rows_h.at[0, :, cols], rows.at[:, cols], KEEP)
        if r == 0:
            load(vel_h, vel, KEEP)
        else:
            near_load.append(load(anchor_h.at[:, cols], anchor.at[:, cols], NEAR + r - 1))

    pl.semaphore_wait(barrier, 1 + y + x + pos)
    for t in range(1, C):
        @pl.when(y >= t)
        def _():
            tell(ready_y, replica=me - 2 * t)

    @pl.when(x == 1)
    def _():
        tell(ready_x, shard=partner)

    for t in range(1, L):
        @pl.when(pos >= t)
        def _():
            tell(ready_z.at[min(t, 2) - 1], shard=at - 2 * t)

    def remote(src, dst, send, recv, **target):
        return pltpu.make_async_remote_copy(
            src_ref=src, dst_ref=dst, send_sem=sends.at[send], recv_sem=recv,
            device_id=target, device_id_type=MESH)

    def whole(ref, semaphore):
        return pltpu.make_async_remote_copy(
            src_ref=ref, dst_ref=ref, send_sem=semaphore, recv_sem=semaphore,
            device_id={"replica": sib}, device_id_type=MESH)

    def sib_copy(j, g):
        cols = columns(2 * j + 1 - c, g * per, per)
        return remote(rows.at[:, cols], sib_rows.at[j, g], 0, sib_recv.at[j, g], replica=sib)

    def more_copy(j):
        cols = columns(2 * j, LOW, EXTRA)
        return remote(rows.at[:, cols], more_rows.at[j], 0, more_recv, replica=sib)

    def more_vel_copy():
        return remote(vel.at[:, pl.ds(LOW * piece, EXTRA * piece)], more_vel, 0, more_recv, replica=sib)

    def cot_copy(k, u, recv, target):
        block = cot.at[tokens(k), pl.ds(u * part_width, part_width)]
        return remote(block, block, 2, recv, shard=target)

    def left_sends():
        for t in range(L - 1, 0, -1):
            @pl.when((pos >= 1) if t == 1 else (pos == L - 1))
            def _():
                for u in range(PARTS):
                    cot_copy(at, u, z_recv.at[t - 1, u], at - 2 * t).start()

    def loaded(count, semaphore):
        cols = pl.ds(0, count * piece)
        pltpu.make_async_copy(rows_h.at[0, :, cols], rows.at[:, cols], in_sem.at[semaphore]).wait()

    loaded(per, FIRST)
    sib_copy(turn(0), 0).start()
    loaded(C * H - per, OUT)
    for r in range(C):
        for g in range(CUTS):
            if r or g:
                sib_copy(turn(r), g).start()
    for q in [2 * turn(0) + c] + [2 * turn(r) + 1 - c for r in range(C)]:
        load(anchor_h.at[:, quarter(q)], anchor.at[:, quarter(q)], REST)
    load(feat_h.at[0], feat, INNER)
    for n, source in enumerate((w_h, m_h, s_h)):
        load(source.at[0], wms.at[n], INNER)
    cot_load.wait()
    pl.when((c == 0) | (pos < L - 1))(left_sends)

    def slot(p, src, j, h):
        return ((p * C + src) * C + j) * H + h

    def message(p, src, j, h):
        return msg.at[slot(p, src, j, h)]

    def y_copy(t, p, j, h, recv):
        return remote(message(p, y, j, h), message(p, y, j, h), 1, recv, replica=lax.rem(me + 2 * t, R))

    def own_to_sib(p, j, h):
        return remote(message(p, y, j, h), message(p, y, j, h), 1, own_recv, replica=sib)

    def to_sib(t, p, j, h, recv):
        src = lax.rem(y + C - t, C)
        return remote(message(p, src, j, h), message(p, src, j, h), 1, recv, replica=sib)

    def more_across(t, j, n):
        block = message(0, y, j, LOW + n)
        return remote(block, block, 1, more_y.at[t - 1, C - 1, n], replica=2 * lax.rem(y + t, C))

    def add_message(p, r, h, other_rows, velocity):
        j = turn(r)
        cols = columns(2 * j + p, h)
        both = rows[:, cols].astype(jnp.float32) + other_rows.astype(jnp.float32)
        if r == 0:
            value = share * both - c2 * velocity
        else:
            value = 2.0 * anchor[:, cols] - both
        msg[slot(p, y, j, h)] = value.astype(jnp.bfloat16)

    goes_around = (y == 1) & (x == 0)
    passes_on = (c == 1) & (y == 0) & (x == 1)

    def around(r, h):
        return C == 2 and r == 0 and h == H - 1

    def pass_copy():
        return pltpu.make_async_remote_copy(
            src_ref=passing, dst_ref=message(1, 1, 1, H - 1), send_sem=in_sem.at[KEEP],
            recv_sem=y_recv.at[0, 0, H - 1], device_id={"shard": partner}, device_id_type=MESH)

    def from_sib(j, h):
        return sib_rows[j, h // per, :, pl.ds(h % per * piece, piece)]

    halves = pl.ds(0, C * W // 2 + W)
    pltpu.make_async_copy(anchor_h.at[:, halves], anchor.at[:, halves], in_sem.at[KEEP]).wait()
    for r in range(C):
        j = turn(r)

        @pl.when(c == 0)
        def _():
            more_copy(j).start()

        if r == 0:
            @pl.when(c == 0)
            def _():
                more_vel_copy().start()
        else:
            near_load[r - 1].wait()

        for h in range(H):
            if h % per == 0:
                sib_copy(j, h // per).wait_recv()

            def handle():
                add_message(c, r, h, from_sib(j, h), vel[:, h * piece:(h + 1) * piece])
                if r == 0 and h == 0:
                    @pl.when(y < C - 1)
                    def _():
                        pl.semaphore_wait(ready_y, C - 1 - y)

                for t in range(1, C):
                    if not around(r, h):
                        y_copy(t, c, j, h, y_recv.at[t - 1, r, h]).start()
                if around(r, h):
                    @pl.when((c == 1) & (x == 0))
                    def _():
                        pl.semaphore_wait(ready_x, 1)

                    @pl.when(goes_around)
                    def _():
                        block = message(1, y, j, h)
                        pltpu.make_async_remote_copy(
                            src_ref=block, dst_ref=passing, send_sem=sends.at[1], recv_sem=pass_recv,
                            device_id=(me - 2, partner), device_id_type=MESH).start()

                    @pl.when(jnp.logical_not(goes_around))
                    def _():
                        y_copy(1, c, j, h, y_recv.at[0, r, h]).start()

                own_to_sib(c, j, h).start()

            if h < LOW:
                handle()
            else:
                pl.when(c == 1)(handle)

    @pl.when((x == 0) if C != 2 else (c == 0) & (x == 0))
    def _():
        pl.semaphore_wait(ready_x, 1)

    pl.when((c == 1) & (pos == L - 1))(left_sends)
    for u in range(PARTS):
        cot_copy(at, u, x_recv, partner).start()

    pltpu.make_async_copy(
        anchor_h.at[:, pl.ds(0, (C + 1) * W)], anchor.at[:, pl.ds(0, (C + 1) * W)], in_sem.at[REST]).wait()

    @pl.when(c == 1)
    def _():
        whole(rows.at[:, pl.ds(0, (C + 2) * EXTRA * piece)], more_recv).wait_recv()
        for r in range(C):
            for n in range(EXTRA):
                h, inner = LOW + n, pl.ds(n * piece, piece)
                add_message(0, r, h, more_rows[turn(r), :, inner], more_vel[:, inner])
                for t in range(1, C):
                    if r == C - 1:
                        more_across(t, turn(r), n).start()
                    y_copy(t, 0, turn(r), h, more_y.at[t - 1, r, n]).start()
                own_to_sib(0, turn(r), h).start()

    @pl.when(pos + 1 < L)
    def _():
        pl.semaphore_wait(ready_z.at[0], 1)
        for u in range(PARTS):
            cot_copy(at, u, z_recv.at[L - 2, u], at + 2).start()

    @pl.when(pos + 2 < L)
    def _():
        pl.semaphore_wait(ready_z.at[1], L - 2 - pos)

    @pl.when(pos == 0)
    def _():
        for t in range(2, L):
            for u in range(PARTS):
                cot_copy(at, u, z_recv.at[L - t - 1, u], at + 2 * t).start()

    def finish(p, j, h):
        cols = columns(2 * j + p, h)
        others = msg[slot(p, lax.rem(j + 1, C), j, h)].astype(jnp.float32)
        for t in range(2, C):
            others = others + msg[slot(p, lax.rem(j + t, C), j, h)].astype(jnp.float32)
        own = msg[slot(p, j, j, h)].astype(jnp.float32)
        new_anchor = (1.0 - 2.0 * share) * anchor[:, cols] + own - share * others
        na_o[:, cols] = new_anchor
        mg_o[0, :, cols] = (
            blend_keep * rows[:, cols].astype(jnp.float32) + (1.0 - blend_keep) * new_anchor
        ).astype(jnp.bfloat16)

    def finish_velocity(r, h):
        if r == C - 1:
            cols = columns(2 * y + c, h)
            part = slice(h * piece, (h + 1) * piece)
            total = 2.0 * anchor[:, cols] - (
                rows[:, cols].astype(jnp.float32) + from_sib(y, h).astype(jnp.float32))
            for t in range(1, C):
                total = total + msg[slot(c, lax.rem(y + t, C), y, h)].astype(jnp.float32)
            nv_o[:, part] = momentum_keep * vel[:, part] + total / R

    def came(r):
        return turn(r + 1)

    def sent(r, t):
        return (r + 1 + t) % C

    def own_piece(r, h, forward):
        for t in range(1, C):
            y_copy(t, c, came(r), h, y_recv.at[t - 1, sent(r, t), h]).wait_recv()
            to_sib(t, c, came(r), h, forward).start()
        finish(c, came(r), h)
        finish_velocity(r, h)

    def more_piece(r, n):
        for t in range(1, C):
            y_copy(t, 0, came(r), LOW + n, more_y.at[t - 1, sent(r, t), n]).wait_recv()
            if sent(r, t) < C - 1:
                to_sib(t, 0, came(r), LOW + n, more_fwd).start()
        finish(0, came(r), LOW + n)

    def more_own(r, n):
        for t in range(1, C):
            if sent(r, t) == C - 1:
                more_across(t, came(r), n).wait_recv()
        finish(0, came(r), LOW + n)
        finish_velocity(r, LOW + n)

    def pieces_from_sib(n, semaphore):
        whole(msg.at[:n], semaphore).wait_recv()

    def low_group(r):
        pieces_from_sib((C - 1) * LOW, in_sem.at[OUT + r])
        for h in range(LOW):
            finish(1 - c, came(r), h)

    def cot_piece(i, u):
        higher = L - 1 - pos
        source = jnp.where(i < higher, pos + i + 1, pos - 1 - (i - higher))
        source = jnp.where(pos == L - 2, pos - 1 - i if i < L - 2 else L - 1, source)
        if i > 0:
            source = jnp.where(pos == 0, L - 1 if i == 1 else i, source)
            source = jnp.where(pos == L - 1, 0 if i == 1 else L - 1 - i, source)
        d = lax.rem(source - pos + L, L)
        k = 2 * source + x
        cot_copy(k, u, z_recv.at[d - 1, u], partner).wait_recv()
        inner = (source > 0) & (source < L - 1)

        @pl.when(inner & (source > pos) & (pos > 0))
        def _():
            cot_copy(k, u, z_recv.at[d, u], at - 2).start()

        @pl.when(inner & (source < pos) & (pos < L - 1))
        def _():
            cot_copy(k, u, z_recv.at[d - 2, u], at + 2).start()

        cot_copy(k, u, x_recv, partner).start()

    def inner_step():
        whole(cot.at[:L * depth], x_recv).wait_recv()
        cols = pl.ds(0, 3 * wms.shape[2] + feat.shape[1] // 2)
        pltpu.make_async_copy(anchor_h.at[:, cols], anchor.at[:, cols], in_sem.at[INNER]).wait()
        tile = min(512, nw_o.shape[2])
        for n in range(nw_o.shape[2] // tile):
            part = slice(n * tile, (n + 1) * tile)
            gradient = jnp.dot(feat[...], cot[:, part], preferred_element_type=jnp.float32)
            new_first = decay_first * wms[1, :, part] + (1.0 - decay_first) * gradient
            new_second = decay_second * wms[2, :, part] + (1.0 - decay_second) * gradient * gradient
            stepped = new_first / first_fix / (jnp.sqrt(new_second / second_fix) + epsilon)
            weight = wms[0, :, part]
            nw_o[0, :, part] = weight - inner_rate * (stepped + weight_decay * weight)
            nm_o[0, :, part] = new_first
            ns_o[0, :, part] = new_second

    low = [(r, h) for r in range(C) for h in range(LOW)]
    todo = [(i, u) for i in range(L - 1) for u in range(PARTS)]
    each = PARTS * -(-(L - 1) // max(len(low) - 2, 1))
    ready = []
    for i, (r, h) in enumerate(low):
        for step in todo[i * each:(i + 1) * each]:
            cot_piece(*step)
        if i == 0:
            @pl.when(c == 0)
            def _():
                pieces_from_sib(C * (H + EXTRA), own_recv)

            @pl.when(c == 1)
            def _():
                pieces_from_sib(C * LOW, own_recv)

        own_piece(r, h, in_sem.at[OUT + r])
        if C == 2 and i == 0:
            @pl.when(passes_on)
            def _():
                whole(passing, pass_recv).wait_recv()
                pass_copy().start()

        if h == LOW - 1:
            ready.append(r)
        if len(ready) > 1 and h == LOW - 2:
            low_group(ready.pop(0))

    @pl.when(c == 1)
    def _():
        for r in range(C):
            for h in range(LOW, H):
                own_piece(r, h, high_fwd)
        for r in range(C - 1):
            for n in range(EXTRA):
                more_piece(r, n)
        for r in ready:
            low_group(r)
        inner_step()
        for n in range(EXTRA):
            more_piece(C - 1, n)

    @pl.when(c == 0)
    def _():
        for r in ready:
            low_group(r)
        pieces_from_sib((C - 1) * C * EXTRA, high_fwd)
        for r in range(C):
            for h in range(LOW, H):
                finish(1, came(r), h)
        inner_step()
        pieces_from_sib((C - 1) * (C - 1) * EXTRA, more_fwd)
        for r in range(C):
            for n in range(EXTRA):
                more_own(r, n)

    whole(cot.at[:(2 * L - 1) * depth], sends.at[2]).wait_send()

    if C == 2:
        @pl.when(passes_on)
        def _():
            pass_copy().wait_send()

    @pl.when(c == 0)
    def _():
        whole(rows.at[:, pl.ds(0, (C * (H + EXTRA) + 2 * EXTRA) * piece)], sends.at[0]).wait_send()
        whole(msg.at[:(2 * C - 1) * C * LOW], sends.at[1]).wait_send()

    @pl.when(c == 1)
    def _():
        whole(sib_rows, sends.at[0]).wait_send()
        whole(msg.at[:(2 * C - 1) * C * (H + EXTRA)], sends.at[1]).wait_send()


def store_kernel(*refs):
    sems = refs[-1]
    count = (len(refs) - 1) // 2
    pairs = list(zip(refs[:count], refs[count:-1]))
    for i, (source, target) in enumerate(pairs):
        rows = source.shape[-2]
        cuts = 1
        for n in range(cuts):
            part = pl.ds(n * (rows // cuts), rows // cuts)
            index = (0, part) if len(source.shape) == 3 else (part,)
            pltpu.make_async_copy(source.at[index], target.at[index], sems.at[i]).start()
    for i, (source, target) in enumerate(pairs):
        pltpu.make_async_copy(source, target, sems.at[i]).wait()


def store(*arrays):
    return pl.pallas_call(
        store_kernel,
        out_shape=tuple(jax.ShapeDtypeStruct(a.shape, a.dtype) for a in arrays),
        in_specs=[pl.BlockSpec(memory_space=pltpu.VMEM)] * len(arrays),
        out_specs=tuple(pl.BlockSpec(memory_space=pltpu.HBM) for _ in arrays),
        scratch_shapes=[pltpu.SemaphoreType.DMA((len(arrays),))],
        compiler_params=pltpu.CompilerParams(vmem_limit_bytes=2**20),
    )(*arrays)


def local(R, S, anchor, replica_rows, outer_velocity, features, cotangent,
          inner_weight, first_moment, second_moment):
    C, L, H = R // 2, S // 2, SPLIT
    height = anchor.shape[0]
    W = outer_velocity.shape[1]
    f32, bf16 = jnp.float32, jnp.bfloat16
    args = (anchor, replica_rows, outer_velocity, features, cotangent,
            inner_weight, first_moment, second_moment)
    outs = (anchor, replica_rows, outer_velocity, inner_weight, first_moment, second_moment)
    dma, regular = pltpu.SemaphoreType.DMA, pltpu.SemaphoreType.REGULAR
    room = 67043328 - sum(a.size * a.dtype.itemsize for a in outs) - 2**16
    results = pl.pallas_call(
        functools.partial(kernel, R, S),
        out_shape=tuple(pltpu.VMEM(a.shape, a.dtype) for a in outs),
        in_specs=[pl.BlockSpec(memory_space=pltpu.HBM)] * len(args),
        out_specs=tuple(pl.BlockSpec(memory_space=pltpu.VMEM) for _ in outs),
        scratch_shapes=[
            pltpu.VMEM(anchor.shape, f32),
            pltpu.VMEM(replica_rows.shape[1:], bf16),
            pltpu.VMEM(outer_velocity.shape, f32),
            pltpu.VMEM(features.shape[1:], bf16),
            pltpu.VMEM((S * cotangent.shape[1], cotangent.shape[2]), bf16),
            pltpu.VMEM((3,) + inner_weight.shape[1:], f32),
            pltpu.VMEM((C, CUTS, height, W // CUTS), bf16),
            pltpu.VMEM((C, height, EXTRA * (W // H)), bf16),
            pltpu.VMEM((height, EXTRA * (W // H)), f32),
            pltpu.VMEM((2 * C * C * (H + EXTRA), height, W // H), bf16),
            pltpu.VMEM((height, W // H), bf16),
            dma((5 + C,)),
            dma((3,)),
            dma((C, CUTS)),
            dma,
            dma((C - 1, C, H)),
            dma((C - 1, C, EXTRA)),
            dma,
            dma((max(L - 1, 1), PARTS)),
            dma,
            regular,
            regular,
            regular((2,)),
        ],
        compiler_params=pltpu.CompilerParams(
            collective_id=0, has_side_effects=True, vmem_limit_bytes=room),
    )(*args)
    return store(*results)


def solution(mesh):
    in_specs = (
        P("shard", None),
        P("replica", "shard", None),
        P("shard", "replica"),
        P("replica", "shard", None),
        P("replica", "shard", None),
        P("replica", "shard", None),
        P("replica", "shard", None),
        P("replica", "shard", None),
    )
    out_specs = (
        P("shard", None),
        P("replica", "shard", None),
        P("shard", "replica"),
        P("replica", "shard", None),
        P("replica", "shard", None),
        P("replica", "shard", None),
    )
    body = functools.partial(local, mesh.shape["replica"], mesh.shape["shard"])
    return jax.shard_map(body, mesh=mesh, in_specs=in_specs, out_specs=out_specs, check_vma=False)
```

```python
import functools

import jax
import jax.numpy as jnp
from jax import lax
from jax.experimental import pallas as pl
from jax.experimental.pallas import tpu as pltpu
from jax.sharding import PartitionSpec as P

momentum_keep = 0.9
outer_rate = 0.7
blend_keep = 0.5
inner_rate = 0.01
decay_first = 0.9
decay_second = 0.95
weight_decay = 0.1
epsilon = 1e-08
first_fix = 1.0 - 0.9**10
second_fix = 1.0 - 0.95**10

MESH = pl.DeviceIdType.MESH
SPLIT = 4
PARTS = 4
CUTS = 4
EXTRA = 1


def kernel(R, S, anchor_h, rows_h, vel_h, feat_h, cot_h, w_h, m_h, s_h,
           na_o, mg_o, nv_o, nw_o, nm_o, ns_o,
           anchor, rows, vel, feat, cot, wms, sib_rows, more_rows, more_vel, msg, passing,
           in_sem, sends, sib_recv, more_recv, y_recv, more_y, pass_recv, z_recv, x_recv, ready_y, ready_x, ready_z):
    C, L, H = R // 2, S // 2, SPLIT
    LOW = H - EXTRA
    me, at = lax.axis_index("replica"), lax.axis_index("shard")
    y, c = me // 2, me % 2
    pos, x = at // 2, at % 2
    sib = me + 1 - 2 * c
    partner = at + 1 - 2 * x
    W = vel.shape[1]
    piece = W // H
    per = H // CUTS
    depth = cot_h.shape[1]
    part_width = cot_h.shape[2] // PARTS
    c1 = outer_rate * (1.0 + momentum_keep)
    c2 = outer_rate * momentum_keep * momentum_keep
    share = c1 / R

    def columns(q, h, count=1):
        return pl.ds(pl.multiple_of(q * W + h * piece, 128), count * piece)

    def quarter(q):
        return columns(q, 0, H)

    def tokens(k):
        return pl.ds(pl.multiple_of(k * depth, depth), depth)

    def turn(r):
        return lax.rem(y + r, C)

    def tell(semaphore, **target):
        pl.semaphore_signal(semaphore, inc=1, device_id=target, device_id_type=MESH)

    FIRST, COT, INNER, REST, KEEP, OUT = range(6)
    NEAR = OUT + 1
    own_recv, high_fwd, more_fwd = in_sem.at[FIRST], in_sem.at[KEEP], in_sem.at[COT]

    def load(src, dst, slot):
        copy = pltpu.make_async_copy(src, dst, in_sem.at[slot])
        copy.start()
        return copy

    first_cols = columns(2 * turn(0) + 1 - c, 0, per)
    load(rows_h.at[0, :, first_cols], rows.at[:, first_cols], FIRST)

    barrier = pltpu.get_barrier_semaphore()
    tell(barrier, replica=sib)
    for t in range(1, C):
        @pl.when(y + t < C)
        def _():
            tell(barrier, replica=me + 2 * t)

    @pl.when(x == 0)
    def _():
        tell(barrier, shard=partner)

    for t in range(1, L):
        @pl.when(pos + t < L)
        def _():
            tell(barrier, shard=at + 2 * t)

    for r in range(C):
        for g in range(CUTS):
            if r or g:
                cols = columns(2 * turn(r) + 1 - c, g * per, per)
                load(rows_h.at[0, :, cols], rows.at[:, cols], OUT)
    cot_load = load(cot_h.at[0], cot.at[tokens(at)], COT)
    near_load = []
    for r in range(C):
        cols = quarter(2 * turn(r) + c)
        load(rows_h.at[0, :, cols], rows.at[:, cols], KEEP)
        if r == 0:
            load(vel_h, vel, KEEP)
        else:
            near_load.append(load(anchor_h.at[:, cols], anchor.at[:, cols], NEAR + r - 1))

    pl.semaphore_wait(barrier, 1 + y + x + pos)
    for t in range(1, C):
        @pl.when(y >= t)
        def _():
            tell(ready_y, replica=me - 2 * t)

    @pl.when(x == 1)
    def _():
        tell(ready_x, shard=partner)

    for t in range(1, L):
        @pl.when(pos >= t)
        def _():
            tell(ready_z.at[min(t, 2) - 1], shard=at - 2 * t)

    def remote(src, dst, send, recv, **target):
        return pltpu.make_async_remote_copy(
            src_ref=src, dst_ref=dst, send_sem=sends.at[send], recv_sem=recv,
            device_id=target, device_id_type=MESH)

    def whole(ref, semaphore):
        return pltpu.make_async_remote_copy(
            src_ref=ref, dst_ref=ref, send_sem=semaphore, recv_sem=semaphore,
            device_id={"replica": sib}, device_id_type=MESH)

    def sib_copy(j, g):
        cols = columns(2 * j + 1 - c, g * per, per)
        return remote(rows.at[:, cols], sib_rows.at[j, g], 0, sib_recv.at[j, g], replica=sib)

    def more_copy(j):
        cols = columns(2 * j, LOW, EXTRA)
        return remote(rows.at[:, cols], more_rows.at[j], 0, more_recv, replica=sib)

    def more_vel_copy():
        return remote(vel.at[:, pl.ds(LOW * piece, EXTRA * piece)], more_vel, 0, more_recv, replica=sib)

    def cot_copy(k, u, recv, target):
        block = cot.at[tokens(k), pl.ds(u * part_width, part_width)]
        return remote(block, block, 2, recv, shard=target)

    def left_sends():
        for t in range(L - 1, 0, -1):
            @pl.when((pos >= 1) if t == 1 else (pos == L - 1))
            def _():
                for u in range(PARTS):
                    cot_copy(at, u, z_recv.at[t - 1, u], at - 2 * t).start()

    def loaded(count, semaphore):
        cols = pl.ds(0, count * piece)
        pltpu.make_async_copy(rows_h.at[0, :, cols], rows.at[:, cols], in_sem.at[semaphore]).wait()

    loaded(per, FIRST)
    sib_copy(turn(0), 0).start()
    loaded(C * H - per, OUT)
    for r in range(C):
        for g in range(CUTS):
            if r or g:
                sib_copy(turn(r), g).start()
    for q in [2 * turn(0) + c] + [2 * turn(r) + 1 - c for r in range(C)]:
        load(anchor_h.at[:, quarter(q)], anchor.at[:, quarter(q)], REST)
    load(feat_h.at[0], feat, INNER)
    for n, source in enumerate((w_h, m_h, s_h)):
        load(source.at[0], wms.at[n], INNER)
    cot_load.wait()
    pl.when((c == 0) | (pos < L - 1))(left_sends)

    def slot(p, src, j, h):
        return ((p * C + src) * C + j) * H + h

    def message(p, src, j, h):
        return msg.at[slot(p, src, j, h)]

    def y_copy(t, p, j, h, recv):
        return remote(message(p, y, j, h), message(p, y, j, h), 1, recv, replica=lax.rem(me + 2 * t, R))

    def own_to_sib(p, j, h):
        return remote(message(p, y, j, h), message(p, y, j, h), 1, own_recv, replica=sib)

    def to_sib(t, p, j, h, recv):
        src = lax.rem(y + C - t, C)
        return remote(message(p, src, j, h), message(p, src, j, h), 1, recv, replica=sib)

    def more_across(t, j, n):
        block = message(0, y, j, LOW + n)
        return remote(block, block, 1, more_y.at[t - 1, C - 1, n], replica=2 * lax.rem(y + t, C))

    def add_message(p, r, h, other_rows, velocity):
        j = turn(r)
        cols = columns(2 * j + p, h)
        both = rows[:, cols].astype(jnp.float32) + other_rows.astype(jnp.float32)
        if r == 0:
            value = share * both - c2 * velocity
        else:
            value = 2.0 * anchor[:, cols] - both
        msg[slot(p, y, j, h)] = value.astype(jnp.bfloat16)

    goes_around = (y == 1) & (x == 0)
    passes_on = (c == 1) & (y == 0) & (x == 1)

    def around(r, h):
        return C == 2 and r == 0 and h == H - 1

    def pass_copy():
        return pltpu.make_async_remote_copy(
            src_ref=passing, dst_ref=message(1, 1, 1, H - 1), send_sem=in_sem.at[KEEP],
            recv_sem=y_recv.at[0, 0, H - 1], device_id={"shard": partner}, device_id_type=MESH)

    def from_sib(j, h):
        return sib_rows[j, h // per, :, pl.ds(h % per * piece, piece)]

    halves = pl.ds(0, C * W // 2 + W)
    pltpu.make_async_copy(anchor_h.at[:, halves], anchor.at[:, halves], in_sem.at[KEEP]).wait()
    for r in range(C):
        j = turn(r)

        @pl.when(c == 0)
        def _():
            more_copy(j).start()

        if r == 0:
            @pl.when(c == 0)
            def _():
                more_vel_copy().start()
        else:
            near_load[r - 1].wait()

        for h in range(H):
            if h % per == 0:
                sib_copy(j, h // per).wait_recv()

            def handle():
                add_message(c, r, h, from_sib(j, h), vel[:, h * piece:(h + 1) * piece])
                if r == 0 and h == 0:
                    @pl.when(y < C - 1)
                    def _():
                        pl.semaphore_wait(ready_y, C - 1 - y)

                for t in range(1, C):
                    if not around(r, h):
                        y_copy(t, c, j, h, y_recv.at[t - 1, r, h]).start()
                if around(r, h):
                    @pl.when((c == 1) & (x == 0))
                    def _():
                        pl.semaphore_wait(ready_x, 1)

                    @pl.when(goes_around)
                    def _():
                        block = message(1, y, j, h)
                        pltpu.make_async_remote_copy(
                            src_ref=block, dst_ref=passing, send_sem=sends.at[1], recv_sem=pass_recv,
                            device_id=(me - 2, partner), device_id_type=MESH).start()

                    @pl.when(jnp.logical_not(goes_around))
                    def _():
                        y_copy(1, c, j, h, y_recv.at[0, r, h]).start()

                own_to_sib(c, j, h).start()

            if h < LOW:
                handle()
            else:
                pl.when(c == 1)(handle)

    @pl.when((x == 0) if C != 2 else (c == 0) & (x == 0))
    def _():
        pl.semaphore_wait(ready_x, 1)

    pl.when((c == 1) & (pos == L - 1))(left_sends)
    for u in range(PARTS):
        cot_copy(at, u, x_recv, partner).start()

    pltpu.make_async_copy(
        anchor_h.at[:, pl.ds(0, (C + 1) * W)], anchor.at[:, pl.ds(0, (C + 1) * W)], in_sem.at[REST]).wait()

    @pl.when(c == 1)
    def _():
        whole(rows.at[:, pl.ds(0, (C + 2) * EXTRA * piece)], more_recv).wait_recv()
        for r in range(C):
            for n in range(EXTRA):
                h, inner = LOW + n, pl.ds(n * piece, piece)
                add_message(0, r, h, more_rows[turn(r), :, inner], more_vel[:, inner])
                for t in range(1, C):
                    if r == C - 1:
                        more_across(t, turn(r), n).start()
                    y_copy(t, 0, turn(r), h, more_y.at[t - 1, r, n]).start()
                own_to_sib(0, turn(r), h).start()

    @pl.when(pos + 1 < L)
    def _():
        pl.semaphore_wait(ready_z.at[0], 1)
        for u in range(PARTS):
            cot_copy(at, u, z_recv.at[L - 2, u], at + 2).start()

    @pl.when(pos + 2 < L)
    def _():
        pl.semaphore_wait(ready_z.at[1], L - 2 - pos)

    @pl.when(pos == 0)
    def _():
        for t in range(2, L):
            for u in range(PARTS):
                cot_copy(at, u, z_recv.at[L - t - 1, u], at + 2 * t).start()

    def finish(p, j, h):
        cols = columns(2 * j + p, h)
        others = msg[slot(p, lax.rem(j + 1, C), j, h)].astype(jnp.float32)
        for t in range(2, C):
            others = others + msg[slot(p, lax.rem(j + t, C), j, h)].astype(jnp.float32)
        own = msg[slot(p, j, j, h)].astype(jnp.float32)
        new_anchor = (1.0 - 2.0 * share) * anchor[:, cols] + own - share * others
        na_o[:, cols] = new_anchor
        mg_o[0, :, cols] = (
            blend_keep * rows[:, cols].astype(jnp.float32) + (1.0 - blend_keep) * new_anchor
        ).astype(jnp.bfloat16)

    def finish_velocity(r, h):
        if r == C - 1:
            cols = columns(2 * y + c, h)
            part = slice(h * piece, (h + 1) * piece)
            total = 2.0 * anchor[:, cols] - (
                rows[:, cols].astype(jnp.float32) + from_sib(y, h).astype(jnp.float32))
            for t in range(1, C):
                total = total + msg[slot(c, lax.rem(y + t, C), y, h)].astype(jnp.float32)
            nv_o[:, part] = momentum_keep * vel[:, part] + total / R

    def came(r):
        return turn(r + 1)

    def sent(r, t):
        return (r + 1 + t) % C

    def own_piece(r, h, forward):
        for t in range(1, C):
            y_copy(t, c, came(r), h, y_recv.at[t - 1, sent(r, t), h]).wait_recv()
            to_sib(t, c, came(r), h, forward).start()
        finish(c, came(r), h)
        finish_velocity(r, h)

    def more_piece(r, n):
        for t in range(1, C):
            y_copy(t, 0, came(r), LOW + n, more_y.at[t - 1, sent(r, t), n]).wait_recv()
            if sent(r, t) < C - 1:
                to_sib(t, 0, came(r), LOW + n, more_fwd).start()
        finish(0, came(r), LOW + n)

    def more_own(r, n):
        for t in range(1, C):
            if sent(r, t) == C - 1:
                more_across(t, came(r), n).wait_recv()
        finish(0, came(r), LOW + n)
        finish_velocity(r, LOW + n)

    def pieces_from_sib(n, semaphore):
        whole(msg.at[:n], semaphore).wait_recv()

    def low_group(r):
        pieces_from_sib((C - 1) * LOW, in_sem.at[OUT + r])
        for h in range(LOW):
            finish(1 - c, came(r), h)

    def cot_piece(i, u):
        higher = L - 1 - pos
        source = jnp.where(i < higher, pos + i + 1, pos - 1 - (i - higher))
        source = jnp.where(pos == L - 2, pos - 1 - i if i < L - 2 else L - 1, source)
        if i > 0:
            source = jnp.where(pos == 0, L - 1 if i == 1 else i, source)
            source = jnp.where(pos == L - 1, 0 if i == 1 else L - 1 - i, source)
        d = lax.rem(source - pos + L, L)
        k = 2 * source + x
        cot_copy(k, u, z_recv.at[d - 1, u], partner).wait_recv()
        inner = (source > 0) & (source < L - 1)

        @pl.when(inner & (source > pos) & (pos > 0))
        def _():
            cot_copy(k, u, z_recv.at[d, u], at - 2).start()

        @pl.when(inner & (source < pos) & (pos < L - 1))
        def _():
            cot_copy(k, u, z_recv.at[d - 2, u], at + 2).start()

        cot_copy(k, u, x_recv, partner).start()

    def inner_step():
        whole(cot.at[:L * depth], x_recv).wait_recv()
        cols = pl.ds(0, 3 * wms.shape[2] + feat.shape[1] // 2)
        pltpu.make_async_copy(anchor_h.at[:, cols], anchor.at[:, cols], in_sem.at[INNER]).wait()
        tile = min(512, nw_o.shape[2])
        for n in range(nw_o.shape[2] // tile):
            part = slice(n * tile, (n + 1) * tile)
            gradient = jnp.dot(feat[...], cot[:, part], preferred_element_type=jnp.float32)
            new_first = decay_first * wms[1, :, part] + (1.0 - decay_first) * gradient
            new_second = decay_second * wms[2, :, part] + (1.0 - decay_second) * gradient * gradient
            stepped = new_first / first_fix / (jnp.sqrt(new_second / second_fix) + epsilon)
            weight = wms[0, :, part]
            nw_o[0, :, part] = weight - inner_rate * (stepped + weight_decay * weight)
            nm_o[0, :, part] = new_first
            ns_o[0, :, part] = new_second

    low = [(r, h) for r in range(C) for h in range(LOW)]
    todo = [(i, u) for i in range(L - 1) for u in range(PARTS)]
    each = PARTS * -(-(L - 1) // max(len(low) - 2, 1))
    ready = []
    for i, (r, h) in enumerate(low):
        for step in todo[i * each:(i + 1) * each]:
            cot_piece(*step)
        if i == 0:
            @pl.when(c == 0)
            def _():
                pieces_from_sib(C * (H + EXTRA), own_recv)

            @pl.when(c == 1)
            def _():
                pieces_from_sib(C * LOW, own_recv)

        own_piece(r, h, in_sem.at[OUT + r])
        if C == 2 and i == 0:
            @pl.when(passes_on)
            def _():
                whole(passing, pass_recv).wait_recv()
                pass_copy().start()

        if h == LOW - 1:
            ready.append(r)
        if len(ready) > 1 and h == LOW - 2:
            low_group(ready.pop(0))

    @pl.when(c == 1)
    def _():
        for r in range(C):
            for h in range(LOW, H):
                own_piece(r, h, high_fwd)
        for r in range(C - 1):
            for n in range(EXTRA):
                more_piece(r, n)
        for r in ready:
            low_group(r)
        inner_step()
        for n in range(EXTRA):
            more_piece(C - 1, n)

    @pl.when(c == 0)
    def _():
        for r in ready:
            low_group(r)
        pieces_from_sib((C - 1) * C * EXTRA, high_fwd)
        for r in range(C):
            for h in range(LOW, H):
                finish(1, came(r), h)
        inner_step()
        pieces_from_sib((C - 1) * (C - 1) * EXTRA, more_fwd)
        for r in range(C):
            for n in range(EXTRA):
                more_own(r, n)

    whole(cot.at[:(2 * L - 1) * depth], sends.at[2]).wait_send()

    if C == 2:
        @pl.when(passes_on)
        def _():
            pass_copy().wait_send()

    @pl.when(c == 0)
    def _():
        whole(rows.at[:, pl.ds(0, (C * (H + EXTRA) + 2 * EXTRA) * piece)], sends.at[0]).wait_send()
        whole(msg.at[:(2 * C - 1) * C * LOW], sends.at[1]).wait_send()

    @pl.when(c == 1)
    def _():
        whole(sib_rows, sends.at[0]).wait_send()
        whole(msg.at[:(2 * C - 1) * C * (H + EXTRA)], sends.at[1]).wait_send()


def store_kernel(*refs):
    sems = refs[-1]
    count = (len(refs) - 1) // 2
    pairs = list(zip(refs[:count], refs[count:-1]))
    for i, (source, target) in enumerate(pairs):
        rows = source.shape[-2]
        cuts = 1
        for n in range(cuts):
            part = pl.ds(n * (rows // cuts), rows // cuts)
            index = (0, part) if len(source.shape) == 3 else (part,)
            pltpu.make_async_copy(source.at[index], target.at[index], sems.at[i]).start()
    for i, (source, target) in enumerate(pairs):
        pltpu.make_async_copy(source, target, sems.at[i]).wait()


def store(*arrays):
    return pl.pallas_call(
        store_kernel,
        out_shape=tuple(jax.ShapeDtypeStruct(a.shape, a.dtype) for a in arrays),
        in_specs=[pl.BlockSpec(memory_space=pltpu.VMEM)] * len(arrays),
        out_specs=tuple(pl.BlockSpec(memory_space=pltpu.HBM) for _ in arrays),
        scratch_shapes=[pltpu.SemaphoreType.DMA((len(arrays),))],
        compiler_params=pltpu.CompilerParams(vmem_limit_bytes=2**20),
    )(*arrays)


def local(R, S, anchor, replica_rows, outer_velocity, features, cotangent,
          inner_weight, first_moment, second_moment):
    C, L, H = R // 2, S // 2, SPLIT
    height = anchor.shape[0]
    W = outer_velocity.shape[1]
    f32, bf16 = jnp.float32, jnp.bfloat16
    args = (anchor, replica_rows, outer_velocity, features, cotangent,
            inner_weight, first_moment, second_moment)
    outs = (anchor, replica_rows, outer_velocity, inner_weight, first_moment, second_moment)
    dma, regular = pltpu.SemaphoreType.DMA, pltpu.SemaphoreType.REGULAR
    room = 67043328 - sum(a.size * a.dtype.itemsize for a in outs) - 2**16
    results = pl.pallas_call(
        functools.partial(kernel, R, S),
        out_shape=tuple(pltpu.VMEM(a.shape, a.dtype) for a in outs),
        in_specs=[pl.BlockSpec(memory_space=pltpu.HBM)] * len(args),
        out_specs=tuple(pl.BlockSpec(memory_space=pltpu.VMEM) for _ in outs),
        scratch_shapes=[
            pltpu.VMEM(anchor.shape, f32),
            pltpu.VMEM(replica_rows.shape[1:], bf16),
            pltpu.VMEM(outer_velocity.shape, f32),
            pltpu.VMEM(features.shape[1:], bf16),
            pltpu.VMEM((S * cotangent.shape[1], cotangent.shape[2]), bf16),
            pltpu.VMEM((3,) + inner_weight.shape[1:], f32),
            pltpu.VMEM((C, CUTS, height, W // CUTS), bf16),
            pltpu.VMEM((C, height, EXTRA * (W // H)), bf16),
            pltpu.VMEM((height, EXTRA * (W // H)), f32),
            pltpu.VMEM((2 * C * C * (H + EXTRA), height, W // H), bf16),
            pltpu.VMEM((height, W // H), bf16),
            dma((5 + C,)),
            dma((3,)),
            dma((C, CUTS)),
            dma,
            dma((C - 1, C, H)),
            dma((C - 1, C, EXTRA)),
            dma,
            dma((max(L - 1, 1), PARTS)),
            dma,
            regular,
            regular,
            regular((2,)),
        ],
        compiler_params=pltpu.CompilerParams(
            collective_id=0, has_side_effects=True, vmem_limit_bytes=room),
    )(*args)
    return store(*results)


def solution(mesh):
    in_specs = (
        P("shard", None),
        P("replica", "shard", None),
        P("shard", "replica"),
        P("replica", "shard", None),
        P("replica", "shard", None),
        P("replica", "shard", None),
        P("replica", "shard", None),
        P("replica", "shard", None),
    )
    out_specs = (
        P("shard", None),
        P("replica", "shard", None),
        P("shard", "replica"),
        P("replica", "shard", None),
        P("replica", "shard", None),
        P("replica", "shard", None),
    )
    body = functools.partial(local, mesh.shape["replica"], mesh.shape["shard"])
    return jax.shard_map(body, mesh=mesh, in_specs=in_specs, out_specs=out_specs, check_vma=False)
```
